256 devices in a mesh: rows: 64 (over z, x, core), cols: 4 (over y).
Axes of the slice: x: 4, y: 4, z: 8, core: 2. Of those that a mesh axis runs over, the one named last changes fastest.
Arguments:
- left_features: bfloat16 [2, 768, 512, 256], P(None, 'rows', 'cols'), may hold values from -6 to 6
- right_features: bfloat16 [2, 768, 512, 256], P(None, 'rows', 'cols'), may hold values from -6 to 6
- conv_weight: bfloat16 [3, 3, 256, 256], replicated, may hold values from -0.125 to 0.125
- conv_bias: float32 [256], replicated, may hold values from -3 to 3
Outputs:
- pyramid_out: float32 [2, 768, 512, 480], P(None, 'rows', 'cols')
The draws below stay inside these ranges and needn't reach their ends.
All inputs are finite; a program needn't handle non-finite values.
Results may differ from the reference program's by a relative error of at most 0.0012.
Values may be sent and summed in bfloat16 or wider, within the bound.
A program may use at most 64 MiB of HBM per device.

```python
import math
import jax
import jax.numpy as jnp
from jax import lax

C = 256
DISP = 256
LEVELS = 4
B = 2
H_FEAT = 768
W_FEAT = 512


def steps_of(own_key, dims, pieces, low, largest):
    loudness, own = 1.0, jax.random.fold_in(own_key, 6)
    for position, shards_of in pieces:
        heights = jnp.exp(jax.random.uniform(jax.random.fold_in(own, position), (shards_of,), jnp.float32, low / len(pieces), largest / len(pieces)))
        loudness = loudness * jnp.repeat(heights, dims[position] // shards_of).reshape([-1 if axis == position else 1 for axis in range(len(dims))])
    return loudness


def noise(stream_key, extent, spread, reach, pieces=(), held_as=jnp.bfloat16):
    values = spread * jax.random.normal(stream_key, extent, jnp.float32)
    if pieces:
        values = values * steps_of(stream_key, extent, pieces, -0.22, 0.18)
    return jnp.clip(values, -reach, reach).astype(held_as)


def setup_inputs(seed: int = 0) -> dict:
    seeds = jax.random.split(jax.random.key(seed), 5)
    left_features = noise(seeds[0], (B, H_FEAT, W_FEAT, C), 1.0, 6.0, ((1, 64), (2, 4)))
    right_features = noise(seeds[1], (B, H_FEAT, W_FEAT, C), 1.0, 6.0, ((1, 64), (2, 4)))
    conv_weight = noise(seeds[2], (3, 3, C, C), (9 * C) ** -0.5, 0.125)
    conv_bias = noise(seeds[3], (C,), 0.5, 3.0, (), jnp.float32)
    return {"left_features": left_features, "right_features": right_features, "conv_weight": conv_weight, "conv_bias": conv_bias}


def conv_block(picture, conv_weight, conv_bias):
    height = picture.shape[0] - 2
    breadth = picture.shape[1] - 2
    channels = picture.shape[2]
    total = jnp.zeros((height * breadth, channels), jnp.float32)
    for row_tap in range(3):
        for col_tap in range(3):
            window = picture[row_tap:row_tap + height, col_tap:col_tap + breadth].reshape(-1, channels)
            total = total + jnp.dot(window, conv_weight[row_tap, col_tap], preferred_element_type=jnp.float32)
    centre = picture[1:-1, 1:-1].reshape(-1, channels).astype(jnp.float32)
    encoded = centre + jax.nn.relu(total + conv_bias.astype(jnp.float32))
    return encoded.astype(jnp.bfloat16).reshape(height, breadth, channels)

def pyramid(scores, span_count, level_count, channels):
    queries = scores.shape[-2]
    across = scores.shape[-1]
    leading = scores.shape[:-2]
    skewed = scores[..., 1:].reshape(leading + (-1,))
    skewed = jnp.pad(skewed, [(0, 0)] * len(leading) + [(0, queries)])
    skewed = skewed.reshape(leading + (queries, across))[..., :span_count][..., ::-1]
    volume = skewed * (1.0 / math.sqrt(channels))
    levels = [volume]
    for level in range(1, level_count):
        pooled = volume.reshape(leading + (queries, span_count >> level, 1 << level)).mean(axis=-1)
        levels.append(pooled)
    return jnp.concatenate(levels, axis=-1)

def reference(left_features, right_features, conv_weight, conv_bias):
    batch, height, breadth, channels = left_features.shape

    def encode(images):
        padded = jnp.pad(images, ((0, 0), (1, 1), (1, 1), (0, 0)))
        return lax.map(lambda picture: conv_block(picture, conv_weight, conv_bias), padded)
    left_out = encode(left_features)
    right_out = encode(right_features)
    right_padded = jnp.pad(right_out, ((0, 0), (0, 0), (DISP, 0), (0, 0)))
    left_rows = left_out.reshape(batch * height, breadth, channels)
    right_rows = right_padded.reshape(batch * height, DISP + breadth, channels)

    def one_row(pair):
        scores = jnp.dot(pair[0], pair[1].T, preferred_element_type=jnp.float32)
        return pyramid(scores, DISP, LEVELS, channels)
    result = lax.map(one_row, (left_rows, right_rows))
    return result.reshape(batch, height, breadth, -1)
```

```python
import functools
import math

import jax
import jax.numpy as jnp
from jax import lax
from jax.experimental import pallas as pl
from jax.experimental.pallas import tpu as pltpu
from jax.sharding import PartitionSpec as P

DISP = 256
LEVELS = 4
MESH = pl.DeviceIdType.MESH
F32 = jnp.float32
BF16 = jnp.bfloat16

DIRECT = 2


def kernel(
    rows_total,
    left_hbm,
    right_hbm,
    weight_hbm,
    bias_ref,
    out_hbm,
    buf,
    weight,
    taps,
    enc,
    got,
    result,
    pool,
    flip,
    edge32,
    edge,
    halo,
    corner32,
    corner,
    halo_corner,
    extra,
    load_sem,
    weight_sem,
    row_send,
    row_recv,
    col_send,
    col_recv,
    corner_send,
    corner_recv,
    own_send,
    relay_send,
    got_recv,
    out_sem,
):
    r = lax.axis_index("rows")
    c = lax.axis_index("cols")
    last = rows_total - 1
    batch, height, width, channels = left_hbm.shape
    images = (right_hbm, left_hbm)
    rows = batch * height
    inner = (height - 2) // 2
    chunks = rows // 2

    def place(j):
        is_inner = j < batch * inner
        b = jnp.where(is_inner, j // inner, j - batch * inner)
        first = jnp.where(is_inner, 1 + 2 * (j % inner), 0)
        second = jnp.where(is_inner, 2 + 2 * (j % inner), height - 1)
        return b, first, second

    def place_row(k):
        b, first, second = place(k // 2)
        return b, jnp.where(k % 2 == 0, first, second)

    def load(image, b):
        return pltpu.make_async_copy(
            images[image].at[b], buf.at[image, b, pl.ds(1, height)], load_sem.at[image, b]
        )

    weight_copy = pltpu.make_async_copy(weight_hbm, weight, weight_sem)
    for b in range(batch):
        load(0, b).start()
    weight_copy.start()
    for b in range(batch):
        load(1, b).start()

    barrier = pltpu.get_barrier_semaphore()
    for step in (1, 3):
        pl.semaphore_signal(
            barrier, inc=1, device_id={"rows": r, "cols": (c + step) % 4}, device_id_type=MESH
        )

    @pl.when(r > 0)
    def _():
        pl.semaphore_signal(barrier, inc=1, device_id={"rows": r - 1, "cols": c}, device_id_type=MESH)

    @pl.when(r < last)
    def _():
        pl.semaphore_signal(barrier, inc=1, device_id={"rows": r + 1, "cols": c}, device_id_type=MESH)

    d = lax.broadcasted_iota(jnp.int32, (2 * DISP, DISP - (DISP >> 3)), 0) % DISP
    lane = lax.broadcasted_iota(jnp.int32, (2 * DISP, DISP - (DISP >> 3)), 1)
    table = jnp.zeros(d.shape, F32)
    start = 0
    for level in range(1, LEVELS):
        size = DISP >> level
        inside = jnp.logical_and(lane >= start, lane < start + size)
        hit = jnp.logical_and(inside, (d >> level) == lane - start)
        table = jnp.where(hit, 1.0 / (1 << level), table)
        start += size
    pool[...] = table.astype(BF16)
    i0 = lax.broadcasted_iota(jnp.int32, (width, width), 0)
    i1 = lax.broadcasted_iota(jnp.int32, (width, width), 1)
    flip[...] = jnp.where(i0 + i1 == width - 1, 1.0, 0.0).astype(BF16)

    @pl.when(r == 0)
    def _():
        buf[:, :, 0] = jnp.zeros((2, batch, width, channels), BF16)

    @pl.when(r == last)
    def _():
        buf[:, :, height + 1] = jnp.zeros((2, batch, width, channels), BF16)

    @pl.when(c == 0)
    def _():
        halo[0] = jnp.zeros(halo.shape[1:], BF16)
        halo_corner[0] = jnp.zeros(halo_corner.shape[1:], BF16)

    @pl.when(c == 3)
    def _():
        halo[1] = jnp.zeros(halo.shape[1:], BF16)
        halo_corner[1] = jnp.zeros(halo_corner.shape[1:], BF16)

    def take_column(image, b, row, side):
        if side == 0:
            return buf[image, b, row, width - 16 : width, :].astype(F32)[15:16]
        return buf[image, b, row, 0:16, :].astype(F32)[0:1]

    def extract(image):
        for b in range(batch):
            load(image, b).wait()
        for side in range(2):
            for b in range(batch):
                for h in range(height):
                    edge32[side, b, h + 1 : h + 2, :] = take_column(image, b, h + 1, side)
            edge[side, image] = edge32[side].astype(BF16)

    def column_copy(side, image):
        return pltpu.make_async_remote_copy(
            src_ref=edge.at[side, image],
            dst_ref=halo.at[side, image],
            send_sem=col_send.at[side, image],
            recv_sem=col_recv.at[side, image],
            device_id={"rows": r, "cols": (c + (1 if side == 0 else 3)) % 4},
            device_id_type=MESH,
        )

    def row_copy(side, image, b):
        source, target, to = (height - 1, 0, r + 1) if side == 0 else (0, height + 1, r - 1)
        return pltpu.make_async_remote_copy(
            src_ref=images[image].at[b, source],
            dst_ref=buf.at[image, b, target],
            send_sem=row_send.at[side, image, b],
            recv_sem=row_recv.at[side, image, b],
            device_id={"rows": to, "cols": c},
            device_id_type=MESH,
        )

    def corner_copy(side):
        return pltpu.make_async_remote_copy(
            src_ref=corner.at[side],
            dst_ref=halo_corner.at[side],
            send_sem=corner_send.at[side],
            recv_sem=corner_recv.at[side],
            device_id={"rows": r, "cols": (c + (1 if side == 0 else 3)) % 4},
            device_id_type=MESH,
        )

    sends_col = (c < 3, c > 0)
    gets_col = (c > 0, c < 3)
    sends_row = (r < last, r > 0)
    gets_row = (r > 0, r < last)

    def each_col(conditions, action):
        for side in range(2):
            @pl.when(conditions[side])
            def _(side=side):
                action(side)

    def each_row(conditions, action):
        for side in range(2):
            @pl.when(conditions[side])
            def _(side=side):
                for image in range(2):
                    for b in range(batch):
                        action(side, image, b)

    extract(0)
    neighbours = 2 + (r > 0).astype(jnp.int32) + (r < last).astype(jnp.int32)
    pl.semaphore_wait(barrier, neighbours)
    each_col(sends_col, lambda side: column_copy(side, 0).start())
    each_row(sends_row, lambda side, image, b: row_copy(side, image, b).start())
    extract(1)
    each_col(sends_col, lambda side: column_copy(side, 1).start())

    def product(image, j, slot):
        b, first, second = place(j)
        parts = [
            jnp.concatenate([buf[image, b, first + tap], buf[image, b, second + tap]], axis=0)
            for tap in range(3)
        ]
        window = jnp.concatenate(parts, axis=1)
        for tap in range(3):
            matrix = weight[:, tap].reshape(3 * channels, channels)
            taps[slot, tap] = jnp.dot(window, matrix, preferred_element_type=F32)

    def from_halo(image):
        each_col(gets_col, lambda side: column_copy(side, image).wait_recv())
        for side in range(2):
            vectors = halo[side, image].reshape(batch * 16, channels)
            for tap in range(3):
                extra[side, tap, image] = jnp.dot(
                    vectors, weight[tap, 2 * side], preferred_element_type=F32
                )

    def corners_out():
        each_row(gets_row, lambda side, image, b: row_copy(side, image, b).wait_recv())
        for side in range(2):
            for image in range(2):
                for b in range(batch):
                    for end in range(2):
                        at = (image * batch + b) * 2 + end
                        corner32[side, at : at + 1, :] = take_column(image, b, end * (height + 1), side)
            corner[side] = corner32[side].astype(BF16)
        each_col(sends_col, lambda side: corner_copy(side).start())

    def corners_add(image):
        for side in range(2):
            for end in range(2):
                values = jnp.dot(
                    halo_corner[side], weight[2 * end, 2 * side], preferred_element_type=F32
                )
                for b in range(batch):
                    at = (image * batch + b) * 2 + end
                    to = b * 16 + end * (height + 1)
                    extra[side, 2 * end, image, to : to + 1, :] = values[at : at + 1]

    def corners_in():
        each_col(gets_col, lambda side: corner_copy(side).wait_recv())
        corners_add(0)

    column = lax.broadcasted_iota(jnp.int32, (width, channels), 0)

    def encoded(image, b, h, slot, half):
        span = pl.ds(half * width, width)
        sides = [
            sum(extra[side, tap, image, pl.ds(b * 16 + h + tap, 1), :] for tap in range(3))
            for side in range(2)
        ]
        before = pltpu.roll(taps[slot, 0, span, :], 1, 0)
        after = pltpu.roll(taps[slot, 2, span, :], width - 1, 0)
        total = jnp.where(column == 0, sides[0], before) + taps[slot, 1, span, :]
        total = total + jnp.where(column == width - 1, sides[1], after) + bias_ref[...]
        return (buf[image, b, h + 1].astype(F32) + jnp.maximum(total, 0.0)).astype(BF16)

    def own_copy(k, f):
        direct = k < DIRECT
        to = jnp.where(c == 0, 1, jnp.where(c == 1, jnp.where(direct, 2, 0), 3))
        return pltpu.make_async_remote_copy(
            src_ref=enc.at[0, f],
            dst_ref=got.at[0, f],
            send_sem=own_send.at[f],
            recv_sem=got_recv.at[0, f],
            device_id={"rows": r, "cols": to},
            device_id_type=MESH,
        )

    def relay_copy(f):
        source = jnp.where(c == 3, 1, 0)
        to = jnp.where(c == 0, 3, jnp.where(c == 2, 3, 2))
        return pltpu.make_async_remote_copy(
            src_ref=got.at[source, f],
            dst_ref=got.at[jnp.where(c == 3, 0, 1), f],
            send_sem=relay_send.at[f],
            recv_sem=got_recv.at[jnp.where(c == 3, 0, 1), f],
            device_id={"rows": r, "cols": to},
            device_id_type=MESH,
        )

    def arrival(which, f):
        return pltpu.make_async_remote_copy(
            src_ref=got.at[which, f],
            dst_ref=got.at[which, f],
            send_sem=relay_send.at[f],
            recv_sem=got_recv.at[which, f],
            device_id={"rows": r, "cols": (c + 1) % 4},
            device_id_type=MESH,
        )

    def relays(k):
        direct = k < DIRECT
        return jnp.logical_or(
            c == 1,
            jnp.logical_or(
                jnp.logical_and(c == 2, direct),
                jnp.logical_and(jnp.logical_or(c == 0, c == 3), jnp.logical_not(direct)),
            ),
        )

    def relay(k):
        b, h = place_row(k)
        f = b * height + h

        @pl.when(relays(k))
        def _():
            arrival(jnp.where(c == 3, 1, 0), f).wait_recv()
            relay_copy(f).start()

    def correlate(k):
        b, h = place_row(k)
        f = b * height + h
        direct = k < DIRECT

        @pl.when(jnp.logical_or(c == 3, jnp.logical_and(c == 2, jnp.logical_not(direct))))
        def _():
            arrival(0, f).wait_recv()

        @pl.when(jnp.logical_or(c == 2, jnp.logical_and(c == 3, direct)))
        def _():
            arrival(1, f).wait_recv()

        query = enc[1, f]
        blocks = []
        for distance, keys in enumerate((enc[0, f], got[0, f], got[1, f])):
            scores = lax.dot_general(
                query, keys, (((1,), (1,)), ((), ())), preferred_element_type=F32
            )
            if distance:
                scores = jnp.where(c >= distance, scores, 0.0)
            blocks.append(pltpu.roll(scores, 1, 1, stride=1, stride_axis=0))
        lower = i1 <= i0
        volume = jnp.concatenate(
            [jnp.where(lower, blocks[0], blocks[1]), jnp.where(lower, blocks[1], blocks[2])], axis=1
        ) * (1.0 / math.sqrt(channels))
        high = volume.astype(BF16)
        low = (volume - high.astype(F32)).astype(BF16)
        result[f, :, 0:DISP] = volume
        result[f, :, DISP:] = jnp.dot(
            jnp.concatenate([high, low], axis=1), pool[...], preferred_element_type=F32
        )
        pltpu.make_async_copy(result.at[f], out_hbm.at[b, h], out_sem.at[f]).start()

    weight_copy.wait()
    product(0, 0, 0)
    from_halo(0)

    def right_chunk(j, _):
        slot = j % 2

        @pl.when(j == 6)
        def _():
            corners_out()

        @pl.when(j == 9)
        def _():
            corners_in()

        following = j + 1
        product_image = following // chunks
        product(product_image, following % chunks, 1 - slot)
        b, first, second = place(j)
        for half, h in enumerate((first, second)):
            value = encoded(0, b, h, slot, half)
            f = b * height + h
            enc[0, f] = jnp.dot(flip[...], value, preferred_element_type=F32).astype(BF16)

        @pl.when(c < 3)
        def _():
            own_copy(2 * j, b * height + first).start()
            own_copy(2 * j + 1, b * height + second).start()

        @pl.when(j == 8)
        def _():
            relay(0)

        @pl.when(j == 11)
        def _():
            relay(1)

        return 0

    lax.fori_loop(0, chunks, right_chunk, 0)
    from_halo(1)
    corners_add(1)

    early = 6

    def left_chunk(j, _):
        slot = (chunks + j) % 2
        product(1, jnp.minimum(j + 1, chunks - 1), 1 - slot)
        b, first, second = place(j)
        for half, h in enumerate((first, second)):
            enc[1, b * height + h] = encoded(1, b, h, slot, half)

        @pl.when(j % 3 == 2)
        def _():
            relay(2 + j // 3)

        return 0

    lax.fori_loop(0, chunks, left_chunk, 0)

    def score_row(k, _):
        @pl.when(k + early < rows)
        def _():
            relay(k + early)

        correlate(k)
        return 0

    lax.fori_loop(0, rows, score_row, 0)

    def drain(k, _):
        b, h = place_row(k)
        f = b * height + h
        pltpu.make_async_copy(result.at[f], out_hbm.at[b, h], out_sem.at[f]).wait()

        @pl.when(c < 3)
        def _():
            own_copy(k, f).wait_send()

        @pl.when(relays(k))
        def _():
            relay_copy(f).wait_send()

        return 0

    each_col(sends_col, lambda side: column_copy(side, 0).wait_send())
    each_col(sends_col, lambda side: column_copy(side, 1).wait_send())
    each_col(sends_col, lambda side: corner_copy(side).wait_send())
    each_row(sends_row, lambda side, image, b: row_copy(side, image, b).wait_send())
    lax.fori_loop(0, rows, drain, 0)


def shards(rows_total, left_features, right_features, conv_weight, conv_bias):
    batch, height, width, channels = left_features.shape
    rows = batch * height
    lanes = sum(DISP >> level for level in range(LEVELS))
    anywhere = pl.BlockSpec(memory_space=pl.ANY)
    dma = pltpu.SemaphoreType.DMA
    return pl.pallas_call(
        functools.partial(kernel, rows_total),
        out_shape=jax.ShapeDtypeStruct((batch, height, width, lanes), F32),
        in_specs=[anywhere, anywhere, anywhere, pl.BlockSpec(memory_space=pltpu.VMEM)],
        out_specs=anywhere,
        scratch_shapes=[
            pltpu.VMEM((2, batch, height + 2, width, channels), BF16),
            pltpu.VMEM((3, 3, channels, channels), BF16),
            pltpu.VMEM((2, 3, 2 * width, channels), F32),
            pltpu.VMEM((2, rows, width, channels), BF16),
            pltpu.VMEM((2, rows, width, channels), BF16),
            pltpu.VMEM((rows, width, lanes), F32),
            pltpu.VMEM((2 * DISP, lanes - DISP), BF16),
            pltpu.VMEM((width, width), BF16),
            pltpu.VMEM((2, batch, 16, channels), F32),
            pltpu.VMEM((2, 2, batch, 16, channels), BF16),
            pltpu.VMEM((2, 2, batch, 16, channels), BF16),
            pltpu.VMEM((2, 16, channels), F32),
            pltpu.VMEM((2, 16, channels), BF16),
            pltpu.VMEM((2, 16, channels), BF16),
            pltpu.VMEM((2, 3, 2, batch * 16, channels), F32),
            dma((2, batch)),
            dma,
            dma((2, 2, batch)),
            dma((2, 2, batch)),
            dma((2, 2)),
            dma((2, 2)),
            dma((2,)),
            dma((2,)),
            dma((rows,)),
            dma((rows,)),
            dma((2, rows)),
            dma((rows,)),
        ],
        compiler_params=pltpu.CompilerParams(
            collective_id=0, has_side_effects=True, vmem_limit_bytes=40 * 1024 * 1024
        ),
    )(left_features, right_features, conv_weight, conv_bias.reshape(1, channels))


def solution(mesh):
    return jax.shard_map(
        functools.partial(shards, mesh.shape["rows"]),
        mesh=mesh,
        in_specs=(P(None, "rows", "cols", None), P(None, "rows", "cols", None), P(), P()),
        out_specs=P(None, "rows", "cols", None),
        check_vma=False,
    )
```

```python
import functools
import math

import jax
import jax.numpy as jnp
from jax import lax
from jax.experimental import pallas as pl
from jax.experimental.pallas import tpu as pltpu
from jax.sharding import PartitionSpec as P

DISP = 256
LEVELS = 4
MESH = pl.DeviceIdType.MESH
F32 = jnp.float32
BF16 = jnp.bfloat16

DIRECT = 2
LAG = 3


def kernel(
    rows_total,
    left_hbm,
    right_hbm,
    weight_hbm,
    bias_hbm,
    result,
    buf,
    weight,
    bias,
    taps,
    enc,
    got,
    pool,
    flip,
    edge32,
    edge,
    halo,
    corner32,
    corner,
    halo_corner,
    extra,
    load_sem,
    weight_sem,
    bias_sem,
    row_send,
    row_recv,
    col_send,
    col_recv,
    corner_send,
    corner_recv,
    own_send,
    relay_send,
    got_recv,
):
    r = lax.axis_index("rows")
    c = lax.axis_index("cols")
    last = rows_total - 1
    batch, height, width, channels = left_hbm.shape
    images = (right_hbm, left_hbm)
    rows = batch * height
    inner = (height - 2) // 2
    chunks = rows // 2

    def place(j):
        is_inner = j < batch * inner
        b = jnp.where(is_inner, j // inner, j - batch * inner)
        first = jnp.where(is_inner, 1 + 2 * (j % inner), 0)
        second = jnp.where(is_inner, 2 + 2 * (j % inner), height - 1)
        return b, first, second

    def place_row(k):
        b, first, second = place(k // 2)
        return b, jnp.where(k % 2 == 0, first, second)

    def load(image, b):
        return pltpu.make_async_copy(
            images[image].at[b], buf.at[image, b, pl.ds(1, height)], load_sem.at[image, b]
        )

    weight_copy = pltpu.make_async_copy(weight_hbm, weight, weight_sem)
    bias_copy = pltpu.make_async_copy(bias_hbm, bias, bias_sem)
    for b in range(batch):
        load(0, b).start()
    weight_copy.start()
    bias_copy.start()
    for b in range(batch):
        load(1, b).start()

    sends_col = (c < 3, c > 0)
    gets_col = (c > 0, c < 3)
    sends_row = (r < last, r > 0)
    gets_row = (r > 0, r < last)
    col_to = ((c + 1) % 4, (c + 3) % 4)
    row_to = (r + 1, r - 1)

    barrier = pltpu.get_barrier_semaphore()

    def greet(row, col):
        pl.semaphore_signal(
            barrier, inc=1, device_id={"rows": row, "cols": col}, device_id_type=MESH
        )

    for side in range(2):
        greet(r, col_to[side])
        for end in range(2):
            pl.when(jnp.logical_and(sends_col[side], sends_row[end]))(
                functools.partial(greet, row_to[end], col_to[side])
            )
    for end in range(2):
        pl.when(sends_row[end])(functools.partial(greet, row_to[end], c))

    d = lax.broadcasted_iota(jnp.int32, (DISP - (DISP >> 3), 2 * DISP), 1) % DISP
    lane = lax.broadcasted_iota(jnp.int32, (DISP - (DISP >> 3), 2 * DISP), 0)
    table = jnp.zeros(d.shape, F32)
    start = 0
    for level in range(1, LEVELS):
        size = DISP >> level
        inside = jnp.logical_and(lane >= start, lane < start + size)
        hit = jnp.logical_and(inside, (d >> level) == lane - start)
        table = jnp.where(hit, 1.0 / (1 << level), table)
        start += size
    pool[...] = table.astype(BF16)
    i0 = lax.broadcasted_iota(jnp.int32, (width, width), 0)
    i1 = lax.broadcasted_iota(jnp.int32, (width, width), 1)
    flip[...] = jnp.where(i0 + i1 == width - 1, 1.0, 0.0).astype(BF16)

    @pl.when(r == 0)
    def _():
        buf[:, :, 0] = jnp.zeros((2, batch, width, channels), BF16)
        halo_corner[:, 0] = jnp.zeros((2, 16, channels), BF16)

    @pl.when(r == last)
    def _():
        buf[:, :, height + 1] = jnp.zeros((2, batch, width, channels), BF16)
        halo_corner[:, 1] = jnp.zeros((2, 16, channels), BF16)

    @pl.when(c == 0)
    def _():
        halo[0] = jnp.zeros(halo.shape[1:], BF16)
        halo_corner[0] = jnp.zeros(halo_corner.shape[1:], BF16)

    @pl.when(c == 3)
    def _():
        halo[1] = jnp.zeros(halo.shape[1:], BF16)
        halo_corner[1] = jnp.zeros(halo_corner.shape[1:], BF16)

    def take_column(image, b, row, side):
        if side == 0:
            return buf[image, b, row, width - 16 : width, :].astype(F32)[15:16]
        return buf[image, b, row, 0:16, :].astype(F32)[0:1]

    def extract(image):
        for b in range(batch):
            load(image, b).wait()
        for side in range(2):
            for b in range(batch):
                for h in range(height):
                    edge32[side, b, h + 1 : h + 2, :] = take_column(image, b, h + 1, side)
            edge[side, image] = edge32[side].astype(BF16)

    def column_copy(side, image):
        return pltpu.make_async_remote_copy(
            src_ref=edge.at[side, image],
            dst_ref=halo.at[side, image],
            send_sem=col_send.at[side, image],
            recv_sem=col_recv.at[side, image],
            device_id={"rows": r, "cols": col_to[side]},
            device_id_type=MESH,
        )

    def row_copy(side, image, b):
        source, target, to = (height - 1, 0, r + 1) if side == 0 else (0, height + 1, r - 1)
        return pltpu.make_async_remote_copy(
            src_ref=images[image].at[b, source],
            dst_ref=buf.at[image, b, target],
            send_sem=row_send.at[side, image, b],
            recv_sem=row_recv.at[side, image, b],
            device_id={"rows": to, "cols": c},
            device_id_type=MESH,
        )

    def corner_copy(side, end):
        return pltpu.make_async_remote_copy(
            src_ref=corner.at[side, end],
            dst_ref=halo_corner.at[side, end],
            send_sem=corner_send.at[side, end],
            recv_sem=corner_recv.at[side, end],
            device_id={"rows": row_to[end], "cols": col_to[side]},
            device_id_type=MESH,
        )

    def each_col(conditions, action):
        for side in range(2):
            @pl.when(conditions[side])
            def _(side=side):
                action(side)

    def each_row(conditions, action):
        for side in range(2):
            @pl.when(conditions[side])
            def _(side=side):
                for image in range(2):
                    for b in range(batch):
                        action(side, image, b)

    def each_corner(col_conditions, row_conditions, action):
        for side in range(2):
            for end in range(2):
                pl.when(jnp.logical_and(col_conditions[side], row_conditions[end]))(
                    functools.partial(action, side, end)
                )

    extract(0)
    beside = (c > 0).astype(jnp.int32) + (c < 3).astype(jnp.int32)
    above = (r > 0).astype(jnp.int32) + (r < last).astype(jnp.int32)
    pl.semaphore_wait(barrier, 2 + above + beside * above)
    each_col(sends_col, lambda side: column_copy(side, 0).start())
    each_row(sends_row, lambda side, image, b: row_copy(side, image, b).start())
    extract(1)
    each_col(sends_col, lambda side: column_copy(side, 1).start())
    for side in range(2):
        for end in range(2):
            for image in range(2):
                for b in range(batch):
                    at = image * batch + b
                    row = 1 if end else height
                    corner32[side, end, at : at + 1, :] = take_column(image, b, row, side)
            corner[side, end] = corner32[side, end].astype(BF16)
    each_corner(sends_col, sends_row, lambda side, end: corner_copy(side, end).start())

    def product(image, j, slot):
        b, first, second = place(j)
        parts = [
            jnp.concatenate([buf[image, b, first + tap], buf[image, b, second + tap]], axis=0)
            for tap in range(3)
        ]
        window = jnp.concatenate(parts, axis=1)
        for tap in range(3):
            matrix = weight[:, tap].reshape(3 * channels, channels)
            taps[slot, tap] = jnp.dot(window, matrix, preferred_element_type=F32)

    def from_halo(image):
        each_col(gets_col, lambda side: column_copy(side, image).wait_recv())
        for side in range(2):
            vectors = halo[side, image].reshape(batch * 16, channels)
            for tap in range(3):
                extra[side, tap, image] = jnp.dot(
                    vectors, weight[tap, 2 * side], preferred_element_type=F32
                )

    def corners_add(image):
        for side in range(2):
            for end in range(2):
                values = jnp.dot(
                    halo_corner[side, end], weight[2 * end, 2 * side], preferred_element_type=F32
                )
                for b in range(batch):
                    at = image * batch + b
                    to = b * 16 + end * (height + 1)
                    extra[side, 2 * end, image, to : to + 1, :] = values[at : at + 1]

    def corners_in():
        each_row(gets_row, lambda side, image, b: row_copy(side, image, b).wait_recv())
        each_corner(gets_col, gets_row, lambda side, end: corner_copy(side, end).wait_recv())
        corners_add(0)

    column = lax.broadcasted_iota(jnp.int32, (width, channels), 0)

    def encoded(image, b, h, slot, half):
        span = pl.ds(half * width, width)
        sides = [
            sum(extra[side, tap, image, pl.ds(b * 16 + h + tap, 1), :] for tap in range(3))
            for side in range(2)
        ]
        before = pltpu.roll(taps[slot, 0, span, :], 1, 0)
        after = pltpu.roll(taps[slot, 2, span, :], width - 1, 0)
        total = jnp.where(column == 0, sides[0], before) + taps[slot, 1, span, :]
        total = total + jnp.where(column == width - 1, sides[1], after) + bias[...]
        return (buf[image, b, h + 1].astype(F32) + jnp.maximum(total, 0.0)).astype(BF16)

    def own_copy(k, f):
        direct = k < DIRECT
        to = jnp.where(c == 0, 1, jnp.where(c == 1, jnp.where(direct, 2, 0), 3))
        return pltpu.make_async_remote_copy(
            src_ref=enc.at[0, f],
            dst_ref=got.at[0, f],
            send_sem=own_send.at[f],
            recv_sem=got_recv.at[0, f],
            device_id={"rows": r, "cols": to},
            device_id_type=MESH,
        )

    def relay_copy(f):
        source = jnp.where(c == 3, 1, 0)
        to = jnp.where(c == 0, 3, jnp.where(c == 2, 3, 2))
        return pltpu.make_async_remote_copy(
            src_ref=got.at[source, f],
            dst_ref=got.at[jnp.where(c == 3, 0, 1), f],
            send_sem=relay_send.at[f],
            recv_sem=got_recv.at[jnp.where(c == 3, 0, 1), f],
            device_id={"rows": r, "cols": to},
            device_id_type=MESH,
        )

    def arrival(which, f):
        return pltpu.make_async_remote_copy(
            src_ref=got.at[which, f],
            dst_ref=got.at[which, f],
            send_sem=relay_send.at[f],
            recv_sem=got_recv.at[which, f],
            device_id={"rows": r, "cols": (c + 1) % 4},
            device_id_type=MESH,
        )

    def relays(k):
        direct = k < DIRECT
        return jnp.logical_or(
            c == 1,
            jnp.logical_or(
                jnp.logical_and(c == 2, direct),
                jnp.logical_and(jnp.logical_or(c == 0, c == 3), jnp.logical_not(direct)),
            ),
        )

    def tick(t):
        k = t + jnp.where(c == 0, DIRECT, jnp.where(c == 3, DIRECT - LAG, 0))
        known = jnp.clip(k, 0, rows - 1)
        b, h = place_row(known)
        f = b * height + h

        @pl.when(jnp.logical_and(k == known, relays(known)))
        def _():
            arrival(jnp.where(c == 3, 1, 0), f).wait_recv()
            relay_copy(f).start()

    def correlate(k):
        b, h = place_row(k)
        f = b * height + h
        direct = k < DIRECT

        @pl.when(jnp.logical_or(c == 3, jnp.logical_and(c == 2, jnp.logical_not(direct))))
        def _():
            arrival(0, f).wait_recv()

        @pl.when(jnp.logical_or(c == 2, jnp.logical_and(c == 3, direct)))
        def _():
            arrival(1, f).wait_recv()

        query = enc[1, f]
        blocks = []
        for distance, keys in enumerate((enc[0, f], got[0, f], got[1, f])):
            scores = lax.dot_general(
                query, keys, (((1,), (1,)), ((), ())), preferred_element_type=F32
            )
            if distance:
                scores = jnp.where(c >= distance, scores, 0.0)
            blocks.append(pltpu.roll(scores, 1, 1, stride=1, stride_axis=0))
        lower = i1 <= i0
        volume = jnp.concatenate(
            [
                jnp.where(lower, blocks[0], blocks[1]).T,
                jnp.where(lower, blocks[1], blocks[2]).T,
            ],
            axis=0,
        ) * (1.0 / math.sqrt(channels))
        high = volume.astype(BF16)
        low = (volume - high.astype(F32)).astype(BF16)
        result[b, h, 0:DISP, :] = volume
        result[b, h, DISP:, :] = jnp.dot(
            pool[...], jnp.concatenate([high, low], axis=0), preferred_element_type=F32
        )

    weight_copy.wait()
    bias_copy.wait()
    product(0, 0, 0)
    from_halo(0)

    def right_chunk(j, _):
        slot = j % 2

        @pl.when(j == 9)
        def _():
            corners_in()

        following = j + 1
        product_image = following // chunks
        product(product_image, following % chunks, 1 - slot)
        b, first, second = place(j)
        for half, h in enumerate((first, second)):
            value = encoded(0, b, h, slot, half)
            f = b * height + h
            enc[0, f] = jnp.dot(flip[...], value, preferred_element_type=F32).astype(BF16)

        @pl.when(c < 3)
        def _():
            own_copy(2 * j, b * height + first).start()
            own_copy(2 * j + 1, b * height + second).start()

        @pl.when(jnp.logical_or(j == 8, j == 11))
        def _():
            tick((j - 8) // 3)

        return 0

    lax.fori_loop(0, chunks, right_chunk, 0)
    from_halo(1)
    corners_add(1)

    early = 2 + chunks // 2

    def left_chunk(j, _):
        slot = (chunks + j) % 2
        product(1, jnp.minimum(j + 1, chunks - 1), 1 - slot)
        b, first, second = place(j)
        for half, h in enumerate((first, second)):
            enc[1, b * height + h] = encoded(1, b, h, slot, half)

        @pl.when(j % 2 == 1)
        def _():
            tick(2 + j // 2)

        return 0

    lax.fori_loop(0, chunks, left_chunk, 0)

    def score_row(k, _):
        tick(k + early)

        correlate((k + DIRECT) % rows)
        return 0

    lax.fori_loop(0, rows, score_row, 0)

    def drain(k, _):
        b, h = place_row(k)
        f = b * height + h

        @pl.when(c < 3)
        def _():
            own_copy(k, f).wait_send()

        @pl.when(relays(k))
        def _():
            relay_copy(f).wait_send()

        return 0

    each_col(sends_col, lambda side: column_copy(side, 0).wait_send())
    each_col(sends_col, lambda side: column_copy(side, 1).wait_send())
    each_corner(sends_col, sends_row, lambda side, end: corner_copy(side, end).wait_send())
    each_row(sends_row, lambda side, image, b: row_copy(side, image, b).wait_send())
    lax.fori_loop(0, rows, drain, 0)


def shards(rows_total, left_features, right_features, conv_weight, conv_bias):
    batch, height, width, channels = left_features.shape
    rows = batch * height
    lanes = sum(DISP >> level for level in range(LEVELS))
    far = pl.BlockSpec(memory_space=pltpu.HBM)
    near = pl.BlockSpec(memory_space=pltpu.VMEM)
    dma = pltpu.SemaphoreType.DMA
    arguments = (left_features, right_features, conv_weight, conv_bias.reshape(1, channels))
    flat = pl.pallas_call(
        functools.partial(kernel, rows_total),
        out_shape=pltpu.VMEM((batch, height, lanes, width), F32),
        in_specs=[far] * 4,
        out_specs=near,
        scratch_shapes=[
            pltpu.VMEM((2, batch, height + 2, width, channels), BF16),
            pltpu.VMEM((3, 3, channels, channels), BF16),
            pltpu.VMEM((1, channels), F32),
            pltpu.VMEM((2, 3, 2 * width, channels), F32),
            pltpu.VMEM((2, rows, width, channels), BF16),
            pltpu.VMEM((2, rows, width, channels), BF16),
            pltpu.VMEM((lanes - DISP, 2 * DISP), BF16),
            pltpu.VMEM((width, width), BF16),
            pltpu.VMEM((2, batch, 16, channels), F32),
            pltpu.VMEM((2, 2, batch, 16, channels), BF16),
            pltpu.VMEM((2, 2, batch, 16, channels), BF16),
            pltpu.VMEM((2, 2, 16, channels), F32),
            pltpu.VMEM((2, 2, 16, channels), BF16),
            pltpu.VMEM((2, 2, 16, channels), BF16),
            pltpu.VMEM((2, 3, 2, batch * 16, channels), F32),
            dma((2, batch)),
            dma,
            dma,
            dma((2, 2, batch)),
            dma((2, 2, batch)),
            dma((2, 2)),
            dma((2, 2)),
            dma((2, 2)),
            dma((2, 2)),
            dma((rows,)),
            dma((rows,)),
            dma((2, rows)),
        ],
        compiler_params=pltpu.CompilerParams(
            collective_id=0, has_side_effects=True, vmem_limit_bytes=40 * 1024 * 1024
        ),
    )(*(pltpu.with_memory_space_constraint(x, pltpu.HBM) for x in arguments))
    return jnp.swapaxes(flat, 2, 3)


def solution(mesh):
    return jax.shard_map(
        functools.partial(shards, mesh.shape["rows"]),
        mesh=mesh,
        in_specs=(P(None, "rows", "cols", None), P(None, "rows", "cols", None), P(), P()),
        out_specs=P(None, "rows", "cols", None),
        check_vma=False,
    )
```

```python
import functools
import math

import jax
import jax.numpy as jnp
from jax import lax
from jax.experimental import pallas as pl
from jax.experimental.pallas import tpu as pltpu
from jax.sharding import PartitionSpec as P

DISP = 256
LEVELS = 4
MESH = pl.DeviceIdType.MESH
F32 = jnp.float32
BF16 = jnp.bfloat16

DIRECT = 2
LAG = 3
EARLY = (4, 5, 6, 8, 9, 10)
PAIRED = 9


def kernel(
    rows_total,
    left_hbm,
    right_hbm,
    weight_hbm,
    bias_hbm,
    result,
    buf,
    weight,
    bias,
    taps,
    enc,
    got,
    pool,
    flip,
    edge32,
    edge,
    halo,
    corner32,
    corner,
    halo_corner,
    extra,
    load_sem,
    weight_sem,
    bias_sem,
    row_send,
    row_recv,
    col_send,
    col_recv,
    corner_send,
    corner_recv,
    own_send,
    relay_send,
    got_recv,
):
    r = lax.axis_index("rows")
    c = lax.axis_index("cols")
    last = rows_total - 1
    batch, height, width, channels = left_hbm.shape
    images = (right_hbm, left_hbm)
    rows = batch * height
    inner = (height - 2) // 2
    chunks = rows // 2

    def place(j):
        is_inner = j < batch * inner
        b = jnp.where(is_inner, j // inner, j - batch * inner)
        first = jnp.where(is_inner, 1 + 2 * (j % inner), 0)
        second = jnp.where(is_inner, 2 + 2 * (j % inner), height - 1)
        return b, first, second

    def place_row(k):
        b, first, second = place(k // 2)
        return b, jnp.where(k % 2 == 0, first, second)

    def load(image):
        return pltpu.make_async_copy(
            images[image], buf.at[image, :, pl.ds(1, height)], load_sem.at[image]
        )

    weight_copy = pltpu.make_async_copy(weight_hbm, weight, weight_sem)
    bias_copy = pltpu.make_async_copy(bias_hbm, bias, bias_sem)
    load(0).start()
    weight_copy.start()
    bias_copy.start()
    load(1).start()

    sends_col = (c < 3, c > 0)
    gets_col = (c > 0, c < 3)
    sends_row = (r < last, r > 0)
    gets_row = (r > 0, r < last)
    col_to = ((c + 1) % 4, (c + 3) % 4)
    row_to = (r + 1, r - 1)

    barrier = pltpu.get_barrier_semaphore()

    def greet(row, col):
        pl.semaphore_signal(
            barrier, inc=1, device_id={"rows": row, "cols": col}, device_id_type=MESH
        )

    for side in range(2):
        greet(r, col_to[side])
    for end in range(2):
        pl.when(sends_row[end])(functools.partial(greet, row_to[end], c))

    d = lax.broadcasted_iota(jnp.int32, (DISP - (DISP >> 3), 2 * DISP), 1) % DISP
    lane = lax.broadcasted_iota(jnp.int32, (DISP - (DISP >> 3), 2 * DISP), 0)
    table = jnp.zeros(d.shape, F32)
    start = 0
    for level in range(1, LEVELS):
        size = DISP >> level
        inside = jnp.logical_and(lane >= start, lane < start + size)
        hit = jnp.logical_and(inside, (d >> level) == lane - start)
        table = jnp.where(hit, 1.0 / (1 << level), table)
        start += size
    pool[...] = table.astype(BF16)
    i0 = lax.broadcasted_iota(jnp.int32, (width, width), 0)
    i1 = lax.broadcasted_iota(jnp.int32, (width, width), 1)
    flip[...] = jnp.where(i0 + i1 == width - 1, 1.0, 0.0).astype(BF16)

    @pl.when(r == 0)
    def _():
        buf[:, :, 0] = jnp.zeros((2, batch, width, channels), BF16)
        halo_corner[0] = jnp.zeros((2, 16, channels), BF16)

    @pl.when(r == last)
    def _():
        buf[:, :, height + 1] = jnp.zeros((2, batch, width, channels), BF16)
        halo_corner[1] = jnp.zeros((2, 16, channels), BF16)

    @pl.when(c == 0)
    def _():
        halo[0] = jnp.zeros(halo.shape[1:], BF16)

    @pl.when(c == 3)
    def _():
        halo[1] = jnp.zeros(halo.shape[1:], BF16)

    def take_column(image, b, row, side):
        if side == 0:
            return buf[image, b, row, width - 16 : width, :].astype(F32)[15:16]
        return buf[image, b, row, 0:16, :].astype(F32)[0:1]

    def extract(image):
        load(image).wait()
        for side in range(2):
            for b in range(batch):
                for h in range(height):
                    edge32[side, b, h + 1 : h + 2, :] = take_column(image, b, h + 1, side)
            edge[side, image] = edge32[side].astype(BF16)

    def column_copy(side, image):
        return pltpu.make_async_remote_copy(
            src_ref=edge.at[side, image],
            dst_ref=halo.at[side, image],
            send_sem=col_send.at[side],
            recv_sem=col_recv.at[side, image],
            device_id={"rows": r, "cols": col_to[side]},
            device_id_type=MESH,
        )

    def row_copy(side, image, b):
        source, target, to = (height - 1, 0, r + 1) if side == 0 else (0, height + 1, r - 1)
        return pltpu.make_async_remote_copy(
            src_ref=images[image].at[b, source],
            dst_ref=buf.at[image, b, target],
            send_sem=row_send.at[side],
            recv_sem=row_recv.at[side],
            device_id={"rows": to, "cols": c},
            device_id_type=MESH,
        )

    def row_copies(side):
        rows_sent = got.at[0, pl.ds(0, 2 * batch)]
        return pltpu.make_async_remote_copy(
            src_ref=rows_sent,
            dst_ref=rows_sent,
            send_sem=row_send.at[side],
            recv_sem=row_recv.at[side],
            device_id={"rows": row_to[side], "cols": c},
            device_id_type=MESH,
        )

    def column_copies(side):
        return pltpu.make_async_remote_copy(
            src_ref=edge.at[side],
            dst_ref=halo.at[side],
            send_sem=col_send.at[side],
            recv_sem=col_recv.at[side, 0],
            device_id={"rows": r, "cols": col_to[side]},
            device_id_type=MESH,
        )

    def corner_copy(end):
        return pltpu.make_async_remote_copy(
            src_ref=corner.at[end],
            dst_ref=halo_corner.at[end],
            send_sem=corner_send.at[end],
            recv_sem=corner_recv.at[end],
            device_id={"rows": row_to[end], "cols": c},
            device_id_type=MESH,
        )

    def each_col(conditions, action):
        for side in range(2):
            @pl.when(conditions[side])
            def _(side=side):
                action(side)

    def each_row(conditions, action):
        for side in range(2):
            @pl.when(conditions[side])
            def _(side=side):
                for image in range(2):
                    for b in range(batch):
                        action(side, image, b)

    extract(0)
    above = (r > 0).astype(jnp.int32) + (r < last).astype(jnp.int32)
    pl.semaphore_wait(barrier, 2 + above)
    each_col(sends_col, lambda side: column_copy(side, 0).start())
    each_row(sends_row, lambda side, image, b: row_copy(side, image, b).start())
    extract(1)
    each_col(sends_col, lambda side: column_copy(side, 1).start())
    def product(image, j, slot):
        b, first, second = place(j)
        parts = [
            jnp.concatenate([buf[image, b, first + tap], buf[image, b, second + tap]], axis=0)
            for tap in range(3)
        ]
        window = jnp.concatenate(parts, axis=1)
        for tap in range(3):
            matrix = weight[:, tap].reshape(3 * channels, channels)
            taps[slot, tap] = jnp.dot(window, matrix, preferred_element_type=F32)

    def from_halo(image):
        for side in range(2):
            vectors = halo[side, image].reshape(batch * 16, channels)
            for tap in range(3):
                extra[side, tap, image] = jnp.dot(
                    vectors, weight[tap, 2 * side], preferred_element_type=F32
                )

    def corners_out():
        each_col(gets_col, lambda side: column_copy(side, 1).wait_recv())
        for end in range(2):
            row = 1 if end else height
            for side in range(2):
                for image in range(2):
                    for b in range(batch):
                        at = image * batch + b
                        vector = halo[side, image, b].astype(F32)[row : row + 1]
                        corner32[end, side, at : at + 1, :] = vector
                corner[end, side] = corner32[end, side].astype(BF16)
        each_col(sends_row, lambda end: corner_copy(end).start())

    def corners_add(image):
        for side in range(2):
            for end in range(2):
                values = jnp.dot(
                    halo_corner[end, side], weight[2 * end, 2 * side], preferred_element_type=F32
                )
                for b in range(batch):
                    at = image * batch + b
                    to = b * 16 + end * (height + 1)
                    extra[side, 2 * end, image, to : to + 1, :] = values[at : at + 1]

    def corners_in():
        each_col(gets_row, lambda side: row_copies(side).wait_recv())
        each_col(gets_row, lambda end: corner_copy(end).wait_recv())
        corners_add(0)

    column = lax.broadcasted_iota(jnp.int32, (width, channels), 0)

    def encoded(image, b, h, slot, half):
        span = pl.ds(half * width, width)
        sides = [
            sum(extra[side, tap, image, pl.ds(b * 16 + h + tap, 1), :] for tap in range(3))
            for side in range(2)
        ]
        before = pltpu.roll(taps[slot, 0, span, :], 1, 0)
        after = pltpu.roll(taps[slot, 2, span, :], width - 1, 0)
        total = jnp.where(column == 0, sides[0], before) + taps[slot, 1, span, :]
        total = total + jnp.where(column == width - 1, sides[1], after) + bias[...]
        return (buf[image, b, h + 1].astype(F32) + jnp.maximum(total, 0.0)).astype(BF16)

    def own_copy(k, f):
        direct = k < DIRECT
        to = jnp.where(c == 0, 1, jnp.where(c == 1, jnp.where(direct, 2, 0), 3))
        return pltpu.make_async_remote_copy(
            src_ref=enc.at[0, f],
            dst_ref=got.at[0, f],
            send_sem=own_send,
            recv_sem=got_recv.at[0, f],
            device_id={"rows": r, "cols": to},
            device_id_type=MESH,
        )

    def relay_copy(f):
        source = jnp.where(c == 3, 1, 0)
        to = jnp.where(c == 0, 3, jnp.where(c == 2, 3, 2))
        return pltpu.make_async_remote_copy(
            src_ref=got.at[source, f],
            dst_ref=got.at[jnp.where(c == 3, 0, 1), f],
            send_sem=relay_send,
            recv_sem=got_recv.at[jnp.where(c == 3, 0, 1), f],
            device_id={"rows": r, "cols": to},
            device_id_type=MESH,
        )

    def arrival(which, f):
        return pltpu.make_async_remote_copy(
            src_ref=got.at[which, f],
            dst_ref=got.at[which, f],
            send_sem=relay_send,
            recv_sem=got_recv.at[which, f],
            device_id={"rows": r, "cols": (c + 1) % 4},
            device_id_type=MESH,
        )

    def relays(k):
        direct = k < DIRECT
        return jnp.logical_or(
            c == 1,
            jnp.logical_or(
                jnp.logical_and(c == 2, direct),
                jnp.logical_and(jnp.logical_or(c == 0, c == 3), jnp.logical_not(direct)),
            ),
        )

    def tick(t):
        k = t + jnp.where(c == 0, DIRECT, jnp.where(c == 3, DIRECT - LAG, 0))
        known = jnp.clip(k, 0, rows - 1)
        b, h = place_row(known)
        f = b * height + h

        @pl.when(jnp.logical_and(k == known, relays(known)))
        def _():
            arrival(jnp.where(c == 3, 1, 0), f).wait_recv()
            relay_copy(f).start()

    def correlate(steps):
        todo = []
        for step in steps:
            k = (step + jnp.where(c == 2, 0, DIRECT)) % rows
            b, h = place_row(k)
            f = b * height + h
            direct = k < DIRECT

            @pl.when(jnp.logical_or(c == 3, jnp.logical_and(c == 2, jnp.logical_not(direct))))
            def _(f=f):
                arrival(0, f).wait_recv()

            @pl.when(jnp.logical_or(c == 2, jnp.logical_and(c == 3, direct)))
            def _(f=f):
                arrival(1, f).wait_recv()

            todo.append((b, h, f))
        lower = i1 <= i0
        for b, h, f in todo:
            query = enc[1, f]
            blocks = []
            for distance, keys in enumerate((enc[0, f], got[0, f], got[1, f])):
                scores = lax.dot_general(
                    query, keys, (((1,), (1,)), ((), ())), preferred_element_type=F32
                )
                if distance:
                    scores = jnp.where(c >= distance, scores, 0.0)
                blocks.append(pltpu.roll(scores, 1, 1, stride=1, stride_axis=0))
            volume = jnp.concatenate(
                [
                    jnp.where(lower, blocks[0], blocks[1]).T,
                    jnp.where(lower, blocks[1], blocks[2]).T,
                ],
                axis=0,
            ) * (1.0 / math.sqrt(channels))
            high = volume.astype(BF16)
            low = (volume - high.astype(F32)).astype(BF16)
            result[b, h, 0:DISP, :] = volume
            result[b, h, DISP:, :] = jnp.dot(
                pool[...], jnp.concatenate([high, low], axis=0), preferred_element_type=F32
            )

    weight_copy.wait()
    bias_copy.wait()
    product(0, 0, 0)
    each_col(gets_col, lambda side: column_copy(side, 0).wait_recv())
    from_halo(0)

    def finish_right(j):
        slot = j % 2
        b, first, second = place(j)
        pair = [encoded(0, b, h, slot, half) for half, h in enumerate((first, second))]
        turned = jnp.dot(flip[...], jnp.concatenate(pair, axis=1), preferred_element_type=F32).astype(BF16)
        for half, h in enumerate((first, second)):
            enc[0, b * height + h] = turned[:, half * channels : (half + 1) * channels]

        @pl.when(c < 3)
        def _():
            own_copy(2 * j, b * height + first).start()
            own_copy(2 * j + 1, b * height + second).start()

    def right_chunk(j, _):
        @pl.when(j == 2)
        def _():
            corners_out()

        @pl.when(j == 9)
        def _():
            corners_in()

        following = j + 1
        product(following // chunks, following % chunks, 1 - j % 2)
        finish_right(j)
        for t, at in enumerate(EARLY):
            pl.when(j == at)(functools.partial(tick, t))
        return 0

    finish_right(0)
    product(0, 1, 1)
    lax.fori_loop(1, chunks, right_chunk, 0)
    from_halo(1)
    corners_add(1)

    early = len(EARLY) + chunks // 2

    def left_chunk(j, _):
        slot = (chunks + j) % 2
        product(1, jnp.minimum(j + 1, chunks - 1), 1 - slot)
        b, first, second = place(j)
        for half, h in enumerate((first, second)):
            enc[1, b * height + h] = encoded(1, b, h, slot, half)

        @pl.when(j % 2 == 0)
        def _():
            tick(len(EARLY) + j // 2)

        return 0

    lax.fori_loop(0, chunks, left_chunk, 0)

    def paired(s, _):
        tick(early + s)
        correlate((2 * s, 2 * s + 1))
        return 0

    def single(step, _):
        tick(early - PAIRED + step)
        correlate((step,))
        return 0

    lax.fori_loop(0, PAIRED, paired, 0)
    lax.fori_loop(2 * PAIRED, rows, single, 0)

    each_col(sends_col, lambda side: column_copies(side).wait_send())
    each_col(sends_row, lambda side: row_copies(side).wait_send())
    each_col(sends_row, lambda end: corner_copy(end).wait_send())

    def drain(sem, count):
        rows_sent = got.at[0, pl.ds(0, count)]
        pltpu.make_async_remote_copy(
            src_ref=rows_sent,
            dst_ref=rows_sent,
            send_sem=sem,
            recv_sem=got_recv.at[0, 0],
            device_id={"rows": r, "cols": (c + 1) % 4},
            device_id_type=MESH,
        ).wait_send()

    pl.when(c < 3)(lambda: drain(own_send, rows))
    pl.when(c == 1)(lambda: drain(relay_send, rows))
    pl.when(c == 2)(lambda: drain(relay_send, DIRECT))
    pl.when(jnp.logical_or(c == 0, c == 3))(lambda: drain(relay_send, rows - DIRECT))


def shards(rows_total, left_features, right_features, conv_weight, conv_bias):
    batch, height, width, channels = left_features.shape
    rows = batch * height
    lanes = sum(DISP >> level for level in range(LEVELS))
    far = pl.BlockSpec(memory_space=pltpu.HBM)
    near = pl.BlockSpec(memory_space=pltpu.VMEM)
    dma = pltpu.SemaphoreType.DMA
    arguments = (left_features, right_features, conv_weight, conv_bias.reshape(1, channels))
    flat = pl.pallas_call(
        functools.partial(kernel, rows_total),
        out_shape=pltpu.VMEM((batch, height, lanes, width), F32),
        in_specs=[far] * 4,
        out_specs=near,
        scratch_shapes=[
            pltpu.VMEM((2, batch, height + 2, width, channels), BF16),
            pltpu.VMEM((3, 3, channels, channels), BF16),
            pltpu.VMEM((1, channels), F32),
            pltpu.VMEM((2, 3, 2 * width, channels), F32),
            pltpu.VMEM((2, rows, width, channels), BF16),
            pltpu.VMEM((2, rows, width, channels), BF16),
            pltpu.VMEM((lanes - DISP, 2 * DISP), BF16),
            pltpu.VMEM((width, width), BF16),
            pltpu.VMEM((2, batch, 16, channels), F32),
            pltpu.VMEM((2, 2, batch, 16, channels), BF16),
            pltpu.VMEM((2, 2, batch, 16, channels), BF16),
            pltpu.VMEM((2, 2, 16, channels), F32),
            pltpu.VMEM((2, 2, 16, channels), BF16),
            pltpu.VMEM((2, 2, 16, channels), BF16),
            pltpu.VMEM((2, 3, 2, batch * 16, channels), F32),
            dma((2,)),
            dma,
            dma,
            dma((2,)),
            dma((2,)),
            dma((2,)),
            dma((2, 2)),
            dma((2,)),
            dma((2,)),
            dma,
            dma,
            dma((2, rows)),
        ],
        compiler_params=pltpu.CompilerParams(
            collective_id=0, has_side_effects=True, vmem_limit_bytes=40 * 1024 * 1024
        ),
    )(*(pltpu.with_memory_space_constraint(x, pltpu.HBM) for x in arguments))
    return jnp.swapaxes(flat, 2, 3)


def solution(mesh):
    return jax.shard_map(
        functools.partial(shards, mesh.shape["rows"]),
        mesh=mesh,
        in_specs=(P(None, "rows", "cols", None), P(None, "rows", "cols", None), P(), P()),
        out_specs=P(None, "rows", "cols", None),
        check_vma=False,
    )
```

```python
import functools
import math

import jax
import jax.numpy as jnp
from jax import lax
from jax.experimental import pallas as pl
from jax.experimental.pallas import tpu as pltpu
from jax.sharding import PartitionSpec as P

DISP = 256
LEVELS = 4
MESH = pl.DeviceIdType.MESH
F32 = jnp.float32
BF16 = jnp.bfloat16

DIRECT = 2
LAG = 3
EARLY = (3, 4, 5, 7, 8, 9, 11)
PAIRED = 9


def kernel(
    rows_total,
    left_hbm,
    right_hbm,
    weight_hbm,
    bias_hbm,
    result,
    buf,
    weight,
    bias,
    taps,
    enc,
    got,
    pool,
    flip,
    edge32,
    edge,
    halo,
    corner32,
    corner,
    halo_corner,
    extra,
    load_sem,
    weight_sem,
    bias_sem,
    row_send,
    row_recv,
    col_send,
    col_recv,
    corner_send,
    corner_recv,
    own_send,
    relay_send,
    got_recv,
):
    r = lax.axis_index("rows")
    c = lax.axis_index("cols")
    last = rows_total - 1
    batch, height, width, channels = left_hbm.shape
    images = (right_hbm, left_hbm)
    rows = batch * height
    inner = (height - 2) // 2
    chunks = rows // 2

    def place(j):
        is_inner = j < batch * inner
        b = jnp.where(is_inner, j // inner, j - batch * inner)
        first = jnp.where(is_inner, 1 + 2 * (j % inner), 0)
        second = jnp.where(is_inner, 2 + 2 * (j % inner), height - 1)
        return b, first, second

    def is_direct(k):
        return jnp.logical_and(k >= DIRECT, k < 2 * DIRECT)

    def round_about(u):
        return jnp.where(u < DIRECT, u, u + DIRECT)

    def place_row(k):
        b, first, second = place(k // 2)
        return b, jnp.where(k % 2 == 0, first, second)

    def load(image):
        return pltpu.make_async_copy(
            images[image], buf.at[image, :, pl.ds(1, height)], load_sem.at[image]
        )

    weight_copy = pltpu.make_async_copy(weight_hbm, weight, weight_sem)
    bias_copy = pltpu.make_async_copy(bias_hbm, bias, bias_sem)
    load(0).start()
    weight_copy.start()
    bias_copy.start()
    load(1).start()

    sends_col = (c < 3, c > 0)
    gets_col = (c > 0, c < 3)
    sends_row = (r < last, r > 0)
    gets_row = (r > 0, r < last)
    col_to = ((c + 1) % 4, (c + 3) % 4)
    row_to = (r + 1, r - 1)

    barrier = pltpu.get_barrier_semaphore()

    def greet(row, col):
        pl.semaphore_signal(
            barrier, inc=1, device_id={"rows": row, "cols": col}, device_id_type=MESH
        )

    for side in range(2):
        greet(r, col_to[side])
    for end in range(2):
        pl.when(sends_row[end])(functools.partial(greet, row_to[end], c))

    d = lax.broadcasted_iota(jnp.int32, (DISP - (DISP >> 3), 2 * DISP), 1) % DISP
    lane = lax.broadcasted_iota(jnp.int32, (DISP - (DISP >> 3), 2 * DISP), 0)
    table = jnp.zeros(d.shape, F32)
    start = 0
    for level in range(1, LEVELS):
        size = DISP >> level
        inside = jnp.logical_and(lane >= start, lane < start + size)
        hit = jnp.logical_and(inside, (d >> level) == lane - start)
        table = jnp.where(hit, 1.0 / (1 << level), table)
        start += size
    pool[...] = table.astype(BF16)
    i0 = lax.broadcasted_iota(jnp.int32, (width, width), 0)
    i1 = lax.broadcasted_iota(jnp.int32, (width, width), 1)
    flip[...] = jnp.where(i0 + i1 == width - 1, 1.0, 0.0).astype(BF16)

    @pl.when(r == 0)
    def _():
        buf[:, :, 0] = jnp.zeros((2, batch, width, channels), BF16)
        halo_corner[0] = jnp.zeros((2, 16, channels), BF16)

    @pl.when(r == last)
    def _():
        buf[:, :, height + 1] = jnp.zeros((2, batch, width, channels), BF16)
        halo_corner[1] = jnp.zeros((2, 16, channels), BF16)

    @pl.when(c == 0)
    def _():
        halo[0] = jnp.zeros(halo.shape[1:], BF16)

    @pl.when(c == 3)
    def _():
        halo[1] = jnp.zeros(halo.shape[1:], BF16)

    def take_column(image, b, row, side):
        if side == 0:
            return buf[image, b, row, width - 16 : width, :].astype(F32)[15:16]
        return buf[image, b, row, 0:16, :].astype(F32)[0:1]

    def extract(image):
        load(image).wait()
        for side in range(2):
            for b in range(batch):
                for h in range(height):
                    edge32[side, b, h + 1 : h + 2, :] = take_column(image, b, h + 1, side)
            edge[side, image] = edge32[side].astype(BF16)

    def column_copy(side, image):
        return pltpu.make_async_remote_copy(
            src_ref=edge.at[side, image],
            dst_ref=halo.at[side, image],
            send_sem=col_send.at[side],
            recv_sem=col_recv.at[side, image],
            device_id={"rows": r, "cols": col_to[side]},
            device_id_type=MESH,
        )

    def row_copy(side, image, b):
        source, target, to = (height - 1, 0, r + 1) if side == 0 else (0, height + 1, r - 1)
        return pltpu.make_async_remote_copy(
            src_ref=images[image].at[b, source],
            dst_ref=buf.at[image, b, target],
            send_sem=row_send.at[side],
            recv_sem=row_recv.at[side],
            device_id={"rows": to, "cols": c},
            device_id_type=MESH,
        )

    def row_copies(side):
        rows_sent = got.at[0, pl.ds(0, 2 * batch)]
        return pltpu.make_async_remote_copy(
            src_ref=rows_sent,
            dst_ref=rows_sent,
            send_sem=row_send.at[side],
            recv_sem=row_recv.at[side],
            device_id={"rows": row_to[side], "cols": c},
            device_id_type=MESH,
        )

    def column_copies(side):
        return pltpu.make_async_remote_copy(
            src_ref=edge.at[side],
            dst_ref=halo.at[side],
            send_sem=col_send.at[side],
            recv_sem=col_recv.at[side, 0],
            device_id={"rows": r, "cols": col_to[side]},
            device_id_type=MESH,
        )

    def corner_copy(end):
        return pltpu.make_async_remote_copy(
            src_ref=corner.at[end],
            dst_ref=halo_corner.at[end],
            send_sem=corner_send.at[end],
            recv_sem=corner_recv.at[end],
            device_id={"rows": row_to[end], "cols": c},
            device_id_type=MESH,
        )

    def each_col(conditions, action):
        for side in range(2):
            @pl.when(conditions[side])
            def _(side=side):
                action(side)

    def each_row(conditions, action):
        for side in range(2):
            @pl.when(conditions[side])
            def _(side=side):
                for image in range(2):
                    for b in range(batch):
                        action(side, image, b)

    extract(0)
    above = (r > 0).astype(jnp.int32) + (r < last).astype(jnp.int32)
    pl.semaphore_wait(barrier, 2 + above)
    each_col(sends_col, lambda side: column_copy(side, 0).start())
    each_row(sends_row, lambda side, image, b: row_copy(side, image, b).start())
    extract(1)
    each_col(sends_col, lambda side: column_copy(side, 1).start())
    def product(image, j, slot):
        b, first, second = place(j)
        parts = [
            jnp.concatenate([buf[image, b, first + tap], buf[image, b, second + tap]], axis=0)
            for tap in range(3)
        ]
        window = jnp.concatenate(parts, axis=1)
        for tap in range(3):
            matrix = weight[:, tap].reshape(3 * channels, channels)
            taps[slot, tap] = jnp.dot(window, matrix, preferred_element_type=F32)

    def from_halo(image):
        for side in range(2):
            vectors = halo[side, image].reshape(batch * 16, channels)
            for tap in range(3):
                extra[side, tap, image] = jnp.dot(
                    vectors, weight[tap, 2 * side], preferred_element_type=F32
                )

    def corners_out():
        each_col(gets_col, lambda side: column_copy(side, 1).wait_recv())
        for end in range(2):
            row = 1 if end else height
            for side in range(2):
                for image in range(2):
                    for b in range(batch):
                        at = image * batch + b
                        vector = halo[side, image, b].astype(F32)[row : row + 1]
                        corner32[end, side, at : at + 1, :] = vector
                corner[end, side] = corner32[end, side].astype(BF16)
        each_col(sends_row, lambda end: corner_copy(end).start())

    def corners_add(image):
        for side in range(2):
            for end in range(2):
                values = jnp.dot(
                    halo_corner[end, side], weight[2 * end, 2 * side], preferred_element_type=F32
                )
                for b in range(batch):
                    at = image * batch + b
                    to = b * 16 + end * (height + 1)
                    extra[side, 2 * end, image, to : to + 1, :] = values[at : at + 1]

    def corners_in():
        each_col(gets_row, lambda side: row_copies(side).wait_recv())
        each_col(gets_row, lambda end: corner_copy(end).wait_recv())
        corners_add(0)

    column = lax.broadcasted_iota(jnp.int32, (width, channels), 0)

    def encoded(image, b, h, slot, half):
        span = pl.ds(half * width, width)
        sides = [
            sum(extra[side, tap, image, pl.ds(b * 16 + h + tap, 1), :] for tap in range(3))
            for side in range(2)
        ]
        before = pltpu.roll(taps[slot, 0, span, :], 1, 0)
        after = pltpu.roll(taps[slot, 2, span, :], width - 1, 0)
        total = jnp.where(column == 0, sides[0], before) + taps[slot, 1, span, :]
        total = total + jnp.where(column == width - 1, sides[1], after) + bias[...]
        return (buf[image, b, h + 1].astype(F32) + jnp.maximum(total, 0.0)).astype(BF16)

    def own_copy(k, f):
        direct = is_direct(k)
        to = jnp.where(c == 0, 1, jnp.where(c == 1, jnp.where(direct, 2, 0), 3))
        return pltpu.make_async_remote_copy(
            src_ref=enc.at[0, f],
            dst_ref=got.at[0, f],
            send_sem=own_send,
            recv_sem=got_recv.at[0, f],
            device_id={"rows": r, "cols": to},
            device_id_type=MESH,
        )

    def relay_copy(f):
        source = jnp.where(c == 3, 1, 0)
        to = jnp.where(c == 0, 3, jnp.where(c == 2, 3, 2))
        return pltpu.make_async_remote_copy(
            src_ref=got.at[source, f],
            dst_ref=got.at[jnp.where(c == 3, 0, 1), f],
            send_sem=relay_send,
            recv_sem=got_recv.at[jnp.where(c == 3, 0, 1), f],
            device_id={"rows": r, "cols": to},
            device_id_type=MESH,
        )

    def arrival(which, f):
        return pltpu.make_async_remote_copy(
            src_ref=got.at[which, f],
            dst_ref=got.at[which, f],
            send_sem=relay_send,
            recv_sem=got_recv.at[which, f],
            device_id={"rows": r, "cols": (c + 1) % 4},
            device_id_type=MESH,
        )

    def relays(k):
        direct = is_direct(k)
        return jnp.logical_or(
            c == 1,
            jnp.logical_or(
                jnp.logical_and(c == 2, direct),
                jnp.logical_and(jnp.logical_or(c == 0, c == 3), jnp.logical_not(direct)),
            ),
        )

    def tick(t):
        k = jnp.where(c == 0, round_about(t), jnp.where(c == 3, round_about(t - LAG), t))
        known = jnp.clip(k, 0, rows - 1)
        b, h = place_row(known)
        f = b * height + h

        @pl.when(jnp.logical_and(k == known, relays(known)))
        def _():
            arrival(jnp.where(c == 3, 1, 0), f).wait_recv()
            relay_copy(f).start()

    def correlate(steps):
        todo = []
        for step in steps:
            late = jnp.where(step < rows - DIRECT, round_about(step), step - (rows - 2 * DIRECT))
            k = jnp.where(c == 2, step, late)
            b, h = place_row(k)
            f = b * height + h
            direct = is_direct(k)

            @pl.when(jnp.logical_or(c == 3, jnp.logical_and(c == 2, jnp.logical_not(direct))))
            def _(f=f):
                arrival(0, f).wait_recv()

            @pl.when(jnp.logical_or(c == 2, jnp.logical_and(c == 3, direct)))
            def _(f=f):
                arrival(1, f).wait_recv()

            todo.append((b, h, f))
        lower = i1 <= i0
        for b, h, f in todo:
            query = enc[1, f]
            blocks = []
            for distance, keys in enumerate((enc[0, f], got[0, f], got[1, f])):
                scores = lax.dot_general(
                    query, keys, (((1,), (1,)), ((), ())), preferred_element_type=F32
                )
                if distance:
                    scores = jnp.where(c >= distance, scores, 0.0)
                blocks.append(pltpu.roll(scores, 1, 1, stride=1, stride_axis=0))
            volume = jnp.concatenate(
                [
                    jnp.where(lower, blocks[0], blocks[1]).T,
                    jnp.where(lower, blocks[1], blocks[2]).T,
                ],
                axis=0,
            ) * (1.0 / math.sqrt(channels))
            high = volume.astype(BF16)
            low = (volume - high.astype(F32)).astype(BF16)
            result[b, h, 0:DISP, :] = volume
            result[b, h, DISP:, :] = jnp.dot(
                pool[...], jnp.concatenate([high, low], axis=0), preferred_element_type=F32
            )

    weight_copy.wait()
    bias_copy.wait()
    product(0, 0, 0)
    each_col(gets_col, lambda side: column_copy(side, 0).wait_recv())
    from_halo(0)

    def finish_right(j):
        slot = j % 2
        b, first, second = place(j)
        pair = [encoded(0, b, h, slot, half) for half, h in enumerate((first, second))]
        turned = jnp.dot(flip[...], jnp.concatenate(pair, axis=1), preferred_element_type=F32).astype(BF16)
        for half, h in enumerate((first, second)):
            enc[0, b * height + h] = turned[:, half * channels : (half + 1) * channels]

        @pl.when(c < 3)
        def _():
            own_copy(2 * j, b * height + first).start()
            own_copy(2 * j + 1, b * height + second).start()

    def right_chunk(j, _):
        @pl.when(j == 2)
        def _():
            corners_out()

        @pl.when(j == 9)
        def _():
            corners_in()

        following = j + 1
        product(following // chunks, following % chunks, 1 - j % 2)
        finish_right(j)
        for t, at in enumerate(EARLY):
            pl.when(j == at)(functools.partial(tick, t))
        return 0

    finish_right(0)
    product(0, 1, 1)
    lax.fori_loop(1, chunks, right_chunk, 0)
    from_halo(1)
    corners_add(1)

    early = len(EARLY) + chunks // 2

    def left_chunk(j, _):
        slot = (chunks + j) % 2
        product(1, jnp.minimum(j + 1, chunks - 1), 1 - slot)
        b, first, second = place(j)
        for half, h in enumerate((first, second)):
            enc[1, b * height + h] = encoded(1, b, h, slot, half)

        @pl.when(j % 2 == 0)
        def _():
            tick(len(EARLY) + j // 2)

        return 0

    lax.fori_loop(0, chunks, left_chunk, 0)

    def paired(s, _):
        tick(early + s)
        correlate((2 * s, 2 * s + 1))
        return 0

    def single(step, _):
        tick(early - PAIRED + step)
        correlate((step,))
        return 0

    lax.fori_loop(0, PAIRED, paired, 0)
    lax.fori_loop(2 * PAIRED, rows, single, 0)

    each_col(sends_col, lambda side: column_copies(side).wait_send())
    each_col(sends_row, lambda side: row_copies(side).wait_send())
    each_col(sends_row, lambda end: corner_copy(end).wait_send())

    def drain(sem, count):
        rows_sent = got.at[0, pl.ds(0, count)]
        pltpu.make_async_remote_copy(
            src_ref=rows_sent,
            dst_ref=rows_sent,
            send_sem=sem,
            recv_sem=got_recv.at[0, 0],
            device_id={"rows": r, "cols": (c + 1) % 4},
            device_id_type=MESH,
        ).wait_send()

    pl.when(c < 3)(lambda: drain(own_send, rows))
    pl.when(c == 1)(lambda: drain(relay_send, rows))
    pl.when(c == 2)(lambda: drain(relay_send, DIRECT))
    pl.when(jnp.logical_or(c == 0, c == 3))(lambda: drain(relay_send, rows - DIRECT))


def shards(rows_total, left_features, right_features, conv_weight, conv_bias):
    batch, height, width, channels = left_features.shape
    rows = batch * height
    lanes = sum(DISP >> level for level in range(LEVELS))
    far = pl.BlockSpec(memory_space=pltpu.HBM)
    near = pl.BlockSpec(memory_space=pltpu.VMEM)
    dma = pltpu.SemaphoreType.DMA
    arguments = (left_features, right_features, conv_weight, conv_bias.reshape(1, channels))
    flat = pl.pallas_call(
        functools.partial(kernel, rows_total),
        out_shape=pltpu.VMEM((batch, height, lanes, width), F32),
        in_specs=[far] * 4,
        out_specs=near,
        scratch_shapes=[
            pltpu.VMEM((2, batch, height + 2, width, channels), BF16),
            pltpu.VMEM((3, 3, channels, channels), BF16),
            pltpu.VMEM((1, channels), F32),
            pltpu.VMEM((2, 3, 2 * width, channels), F32),
            pltpu.VMEM((2, rows, width, channels), BF16),
            pltpu.VMEM((2, rows, width, channels), BF16),
            pltpu.VMEM((lanes - DISP, 2 * DISP), BF16),
            pltpu.VMEM((width, width), BF16),
            pltpu.VMEM((2, batch, 16, channels), F32),
            pltpu.VMEM((2, 2, batch, 16, channels), BF16),
            pltpu.VMEM((2, 2, batch, 16, channels), BF16),
            pltpu.VMEM((2, 2, 16, channels), F32),
            pltpu.VMEM((2, 2, 16, channels), BF16),
            pltpu.VMEM((2, 2, 16, channels), BF16),
            pltpu.VMEM((2, 3, 2, batch * 16, channels), F32),
            dma((2,)),
            dma,
            dma,
            dma((2,)),
            dma((2,)),
            dma((2,)),
            dma((2, 2)),
            dma((2,)),
            dma((2,)),
            dma,
            dma,
            dma((2, rows)),
        ],
        compiler_params=pltpu.CompilerParams(
            collective_id=0, has_side_effects=True, vmem_limit_bytes=40 * 1024 * 1024
        ),
    )(*(pltpu.with_memory_space_constraint(x, pltpu.HBM) for x in arguments))
    return jnp.swapaxes(flat, 2, 3)


def solution(mesh):
    return jax.shard_map(
        functools.partial(shards, mesh.shape["rows"]),
        mesh=mesh,
        in_specs=(P(None, "rows", "cols", None), P(None, "rows", "cols", None), P(), P()),
        out_specs=P(None, "rows", "cols", None),
        check_vma=False,
    )
```

```python
import functools
import math

import jax
import jax.numpy as jnp
from jax import lax
from jax.experimental import pallas as pl
from jax.experimental.pallas import tpu as pltpu
from jax.sharding import PartitionSpec as P

DISP = 256
LEVELS = 4
MESH = pl.DeviceIdType.MESH
F32 = jnp.float32
BF16 = jnp.bfloat16

DIRECT = 2
LAG = 3
EARLY = (3, 4, 5, 7, 8, 9, 11)
PAIRED = 9


def kernel(
    rows_total,
    left_hbm,
    right_hbm,
    weight_hbm,
    bias_hbm,
    result,
    buf,
    weight,
    bias,
    taps,
    enc,
    got,
    pool,
    flip,
    edge32,
    edge,
    halo,
    corner32,
    corner,
    halo_corner,
    extra,
    load_sem,
    weight_sem,
    bias_sem,
    row_send,
    row_recv,
    col_send,
    col_recv,
    corner_send,
    corner_recv,
    own_send,
    relay_send,
    got_recv,
):
    r = lax.axis_index("rows")
    c = lax.axis_index("cols")
    last = rows_total - 1
    batch, height, width, channels = left_hbm.shape
    images = (right_hbm, left_hbm)
    rows = batch * height
    inner = (height - 2) // 2
    chunks = rows // 2

    def place(j):
        is_inner = j < batch * inner
        b = jnp.where(is_inner, j // inner, j - batch * inner)
        first = jnp.where(is_inner, 1 + 2 * (j % inner), 0)
        second = jnp.where(is_inner, 2 + 2 * (j % inner), height - 1)
        return b, first, second

    def is_direct(k):
        return jnp.logical_and(k >= DIRECT, k < 2 * DIRECT)

    def round_about(u):
        return jnp.where(u < DIRECT, u, u + DIRECT)

    def place_row(k):
        b, first, second = place(k // 2)
        return b, jnp.where(k % 2 == 0, first, second)

    def load(image):
        return pltpu.make_async_copy(
            images[image], buf.at[image, :, pl.ds(1, height)], load_sem.at[image]
        )

    weight_copy = pltpu.make_async_copy(weight_hbm, weight, weight_sem)
    bias_copy = pltpu.make_async_copy(bias_hbm, bias, bias_sem)
    load(0).start()
    weight_copy.start()
    bias_copy.start()
    load(1).start()

    sends_col = (c < 3, c > 0)
    gets_col = (c > 0, c < 3)
    sends_row = (r < last, r > 0)
    gets_row = (r > 0, r < last)
    col_to = ((c + 1) % 4, (c + 3) % 4)
    row_to = (r + 1, r - 1)

    barrier = pltpu.get_barrier_semaphore()

    def greet(row, col):
        pl.semaphore_signal(
            barrier, inc=1, device_id={"rows": row, "cols": col}, device_id_type=MESH
        )

    for side in range(2):
        greet(r, col_to[side])
    for end in range(2):
        pl.when(sends_row[end])(functools.partial(greet, row_to[end], c))

    d = lax.broadcasted_iota(jnp.int32, (DISP - (DISP >> 3), 2 * DISP), 1) % DISP
    lane = lax.broadcasted_iota(jnp.int32, (DISP - (DISP >> 3), 2 * DISP), 0)
    table = jnp.zeros(d.shape, F32)
    start = 0
    for level in range(1, LEVELS):
        size = DISP >> level
        inside = jnp.logical_and(lane >= start, lane < start + size)
        hit = jnp.logical_and(inside, (d >> level) == lane - start)
        table = jnp.where(hit, 1.0 / (1 << level), table)
        start += size
    pool[...] = table.astype(BF16)
    i0 = lax.broadcasted_iota(jnp.int32, (width, width), 0)
    i1 = lax.broadcasted_iota(jnp.int32, (width, width), 1)
    flip[...] = jnp.where(i0 + i1 == width - 1, 1.0, 0.0).astype(BF16)

    @pl.when(r == 0)
    def _():
        buf[:, :, 0] = jnp.zeros((2, batch, width, channels), BF16)
        halo_corner[0] = jnp.zeros((2, 16, channels), BF16)

    @pl.when(r == last)
    def _():
        buf[:, :, height + 1] = jnp.zeros((2, batch, width, channels), BF16)
        halo_corner[1] = jnp.zeros((2, 16, channels), BF16)

    @pl.when(c == 0)
    def _():
        halo[0] = jnp.zeros(halo.shape[1:], BF16)

    @pl.when(c == 3)
    def _():
        halo[1] = jnp.zeros(halo.shape[1:], BF16)

    def take_column(image, b, row, side):
        if side == 0:
            return buf[image, b, row, width - 16 : width, :].astype(F32)[15:16]
        return buf[image, b, row, 0:16, :].astype(F32)[0:1]

    def extract(image):
        load(image).wait()
        for side in range(2):
            for b in range(batch):
                for h in range(height):
                    edge32[side, b, h + 1 : h + 2, :] = take_column(image, b, h + 1, side)
            edge[side, image] = edge32[side].astype(BF16)

    def column_copy(side, image):
        return pltpu.make_async_remote_copy(
            src_ref=edge.at[side, image],
            dst_ref=halo.at[side, image],
            send_sem=col_send.at[side],
            recv_sem=col_recv.at[side, image],
            device_id={"rows": r, "cols": col_to[side]},
            device_id_type=MESH,
        )

    def row_copy(side, image, b):
        source, target, to = (height - 1, 0, r + 1) if side == 0 else (0, height + 1, r - 1)
        return pltpu.make_async_remote_copy(
            src_ref=images[image].at[b, source],
            dst_ref=buf.at[image, b, target],
            send_sem=row_send.at[side],
            recv_sem=row_recv.at[side],
            device_id={"rows": to, "cols": c},
            device_id_type=MESH,
        )

    def row_copies(side):
        rows_sent = got.at[0, pl.ds(0, 2 * batch)]
        return pltpu.make_async_remote_copy(
            src_ref=rows_sent,
            dst_ref=rows_sent,
            send_sem=row_send.at[side],
            recv_sem=row_recv.at[side],
            device_id={"rows": row_to[side], "cols": c},
            device_id_type=MESH,
        )

    def column_copies(side):
        return pltpu.make_async_remote_copy(
            src_ref=edge.at[side],
            dst_ref=halo.at[side],
            send_sem=col_send.at[side],
            recv_sem=col_recv.at[side, 0],
            device_id={"rows": r, "cols": col_to[side]},
            device_id_type=MESH,
        )

    def corner_copy(end):
        return pltpu.make_async_remote_copy(
            src_ref=corner.at[end],
            dst_ref=halo_corner.at[end],
            send_sem=corner_send.at[end],
            recv_sem=corner_recv.at[end],
            device_id={"rows": row_to[end], "cols": c},
            device_id_type=MESH,
        )

    def each_col(conditions, action):
        for side in range(2):
            @pl.when(conditions[side])
            def _(side=side):
                action(side)

    def each_row(conditions, action):
        for side in range(2):
            @pl.when(conditions[side])
            def _(side=side):
                for image in range(2):
                    for b in range(batch):
                        action(side, image, b)

    extract(0)
    above = (r > 0).astype(jnp.int32) + (r < last).astype(jnp.int32)
    pl.semaphore_wait(barrier, 2 + above)
    each_col(sends_col, lambda side: column_copy(side, 0).start())
    each_row(sends_row, lambda side, image, b: row_copy(side, image, b).start())
    extract(1)
    each_col(sends_col, lambda side: column_copy(side, 1).start())
    def product(image, j, slot):
        b, first, second = place(j)
        parts = [
            jnp.concatenate([buf[image, b, first + tap], buf[image, b, second + tap]], axis=0)
            for tap in range(3)
        ]
        window = jnp.concatenate(parts, axis=1)
        for tap in range(3):
            matrix = weight[:, tap].reshape(3 * channels, channels)
            taps[slot, tap] = jnp.dot(window, matrix, preferred_element_type=F32)

    def from_halo(image):
        for side in range(2):
            vectors = halo[side, image].reshape(batch * 16, channels)
            for tap in range(3):
                extra[side, tap, image] = jnp.dot(
                    vectors, weight[tap, 2 * side], preferred_element_type=F32
                )

    def corners_out():
        each_col(gets_col, lambda side: column_copy(side, 1).wait_recv())
        for end in range(2):
            row = 1 if end else height
            for side in range(2):
                for image in range(2):
                    for b in range(batch):
                        at = image * batch + b
                        vector = halo[side, image, b].astype(F32)[row : row + 1]
                        corner32[end, side, at : at + 1, :] = vector
                corner[end, side] = corner32[end, side].astype(BF16)
        each_col(sends_row, lambda end: corner_copy(end).start())

    def corners_add(image):
        for side in range(2):
            for end in range(2):
                values = jnp.dot(
                    halo_corner[end, side], weight[2 * end, 2 * side], preferred_element_type=F32
                )
                for b in range(batch):
                    at = image * batch + b
                    to = b * 16 + end * (height + 1)
                    extra[side, 2 * end, image, to : to + 1, :] = values[at : at + 1]

    def corners_in():
        each_col(gets_row, lambda side: row_copies(side).wait_recv())
        each_col(gets_row, lambda end: corner_copy(end).wait_recv())
        corners_add(0)

    column = lax.broadcasted_iota(jnp.int32, (width, channels), 0)

    def encoded(image, b, h, slot, half):
        span = pl.ds(half * width, width)
        sides = [
            sum(extra[side, tap, image, pl.ds(b * 16 + h + tap, 1), :] for tap in range(3))
            for side in range(2)
        ]
        before = pltpu.roll(taps[slot, 0, span, :], 1, 0)
        after = pltpu.roll(taps[slot, 2, span, :], width - 1, 0)
        total = jnp.where(column == 0, sides[0], before) + taps[slot, 1, span, :]
        total = total + jnp.where(column == width - 1, sides[1], after) + bias[...]
        return (buf[image, b, h + 1].astype(F32) + jnp.maximum(total, 0.0)).astype(BF16)

    def piece(ref, which, f, part):
        if part is None:
            return ref.at[which, f]
        return ref.at[which, rows - 1, pl.ds(part * (width // 2), width // 2)]

    def landed(which, f, part):
        return got_recv.at[which, f if part is None else rows - 1 + part]

    def own_copy(k, f, part=None):
        to = jnp.where(c == 0, 1, jnp.where(c == 1, jnp.where(is_direct(k), 2, 0), 3))
        return pltpu.make_async_remote_copy(
            src_ref=piece(enc, 0, f, part),
            dst_ref=piece(got, 0, f, part),
            send_sem=own_send,
            recv_sem=landed(0, f, part),
            device_id={"rows": r, "cols": to},
            device_id_type=MESH,
        )

    def relay_copy(f, part=None):
        source = jnp.where(c == 3, 1, 0)
        target = jnp.where(c == 3, 0, 1)
        to = jnp.where(c == 0, 3, jnp.where(c == 2, 3, 2))
        return pltpu.make_async_remote_copy(
            src_ref=piece(got, source, f, part),
            dst_ref=piece(got, target, f, part),
            send_sem=relay_send,
            recv_sem=landed(target, f, part),
            device_id={"rows": r, "cols": to},
            device_id_type=MESH,
        )

    def arrival(which, f, part=None):
        return pltpu.make_async_remote_copy(
            src_ref=piece(got, which, f, part),
            dst_ref=piece(got, which, f, part),
            send_sem=relay_send,
            recv_sem=landed(which, f, part),
            device_id={"rows": r, "cols": (c + 1) % 4},
            device_id_type=MESH,
        )

    def in_pieces(condition, k, f, action):
        @pl.when(jnp.logical_and(condition, k < rows - 1))
        def _():
            action(f, None)

        @pl.when(jnp.logical_and(condition, k == rows - 1))
        def _():
            for part in range(2):
                action(f, part)

    def relays(k):
        direct = is_direct(k)
        return jnp.logical_or(
            c == 1,
            jnp.logical_or(
                jnp.logical_and(c == 2, direct),
                jnp.logical_and(jnp.logical_or(c == 0, c == 3), jnp.logical_not(direct)),
            ),
        )

    def tick(t):
        k = jnp.where(c == 0, round_about(t), jnp.where(c == 3, round_about(t - LAG), t))
        known = jnp.clip(k, 0, rows - 1)
        b, h = place_row(known)
        f = b * height + h

        def action(f, part):
            arrival(jnp.where(c == 3, 1, 0), f, part).wait_recv()
            relay_copy(f, part).start()

        in_pieces(jnp.logical_and(k == known, relays(known)), known, f, action)

    def correlate(steps):
        todo = []
        for step in steps:
            late = jnp.where(step < rows - DIRECT, round_about(step), step - (rows - 2 * DIRECT))
            k = jnp.where(c == 2, step, late)
            b, h = place_row(k)
            f = b * height + h
            direct = is_direct(k)

            near = jnp.logical_or(c == 3, jnp.logical_and(c == 2, jnp.logical_not(direct)))
            in_pieces(near, k, f, lambda f, part: arrival(0, f, part).wait_recv())
            distant = jnp.logical_or(c == 2, jnp.logical_and(c == 3, direct))
            in_pieces(distant, k, f, lambda f, part: arrival(1, f, part).wait_recv())
            todo.append((b, h, f))
        lower = i1 <= i0
        for b, h, f in todo:
            query = enc[1, f]
            blocks = []
            for distance, keys in enumerate((enc[0, f], got[0, f], got[1, f])):
                scores = lax.dot_general(
                    query, keys, (((1,), (1,)), ((), ())), preferred_element_type=F32
                )
                if distance:
                    scores = jnp.where(c >= distance, scores, 0.0)
                blocks.append(pltpu.roll(scores, 1, 1, stride=1, stride_axis=0))
            volume = jnp.concatenate(
                [
                    jnp.where(lower, blocks[0], blocks[1]).T,
                    jnp.where(lower, blocks[1], blocks[2]).T,
                ],
                axis=0,
            ) * (1.0 / math.sqrt(channels))
            high = volume.astype(BF16)
            low = (volume - high.astype(F32)).astype(BF16)
            result[b, h, 0:DISP, :] = volume
            result[b, h, DISP:, :] = jnp.dot(
                pool[...], jnp.concatenate([high, low], axis=0), preferred_element_type=F32
            )

    weight_copy.wait()
    bias_copy.wait()
    product(0, 0, 0)
    each_col(gets_col, lambda side: column_copy(side, 0).wait_recv())
    from_halo(0)

    def finish_right(j):
        slot = j % 2
        b, first, second = place(j)
        pair = [encoded(0, b, h, slot, half) for half, h in enumerate((first, second))]
        turned = jnp.dot(flip[...], jnp.concatenate(pair, axis=1), preferred_element_type=F32).astype(BF16)
        for half, h in enumerate((first, second)):
            enc[0, b * height + h] = turned[:, half * channels : (half + 1) * channels]

        for half, h in enumerate((first, second)):
            k = 2 * j + half
            in_pieces(c < 3, k, b * height + h, lambda f, part, k=k: own_copy(k, f, part).start())

    def right_chunk(j, _):
        @pl.when(j == 2)
        def _():
            corners_out()

        @pl.when(j == 9)
        def _():
            corners_in()

        following = j + 1
        product(following // chunks, following % chunks, 1 - j % 2)
        finish_right(j)
        for t, at in enumerate(EARLY):
            pl.when(j == at)(functools.partial(tick, t))
        return 0

    finish_right(0)
    product(0, 1, 1)
    lax.fori_loop(1, chunks, right_chunk, 0)
    from_halo(1)
    corners_add(1)

    early = len(EARLY) + chunks // 2

    def left_chunk(j, _):
        slot = (chunks + j) % 2
        product(1, jnp.minimum(j + 1, chunks - 1), 1 - slot)
        b, first, second = place(j)
        for half, h in enumerate((first, second)):
            enc[1, b * height + h] = encoded(1, b, h, slot, half)

        @pl.when(j % 2 == 0)
        def _():
            tick(len(EARLY) + j // 2)

        return 0

    lax.fori_loop(0, chunks, left_chunk, 0)

    def paired(s, _):
        tick(early + s)
        correlate((2 * s, 2 * s + 1))
        return 0

    def single(step, _):
        tick(early - PAIRED + step)
        correlate((step,))
        return 0

    lax.fori_loop(0, PAIRED, paired, 0)
    lax.fori_loop(2 * PAIRED, rows, single, 0)

    each_col(sends_col, lambda side: column_copies(side).wait_send())
    each_col(sends_row, lambda side: row_copies(side).wait_send())
    each_col(sends_row, lambda end: corner_copy(end).wait_send())

    def drain(sem, count):
        rows_sent = got.at[0, pl.ds(0, count)]
        pltpu.make_async_remote_copy(
            src_ref=rows_sent,
            dst_ref=rows_sent,
            send_sem=sem,
            recv_sem=got_recv.at[0, 0],
            device_id={"rows": r, "cols": (c + 1) % 4},
            device_id_type=MESH,
        ).wait_send()

    pl.when(c < 3)(lambda: drain(own_send, rows))
    pl.when(c == 1)(lambda: drain(relay_send, rows))
    pl.when(c == 2)(lambda: drain(relay_send, DIRECT))
    pl.when(jnp.logical_or(c == 0, c == 3))(lambda: drain(relay_send, rows - DIRECT))


def shards(rows_total, left_features, right_features, conv_weight, conv_bias):
    batch, height, width, channels = left_features.shape
    rows = batch * height
    lanes = sum(DISP >> level for level in range(LEVELS))
    far = pl.BlockSpec(memory_space=pltpu.HBM)
    near = pl.BlockSpec(memory_space=pltpu.VMEM)
    dma = pltpu.SemaphoreType.DMA
    arguments = (left_features, right_features, conv_weight, conv_bias.reshape(1, channels))
    flat = pl.pallas_call(
        functools.partial(kernel, rows_total),
        out_shape=pltpu.VMEM((batch, height, lanes, width), F32),
        in_specs=[far] * 4,
        out_specs=near,
        scratch_shapes=[
            pltpu.VMEM((2, batch, height + 2, width, channels), BF16),
            pltpu.VMEM((3, 3, channels, channels), BF16),
            pltpu.VMEM((1, channels), F32),
            pltpu.VMEM((2, 3, 2 * width, channels), F32),
            pltpu.VMEM((2, rows, width, channels), BF16),
            pltpu.VMEM((2, rows, width, channels), BF16),
            pltpu.VMEM((lanes - DISP, 2 * DISP), BF16),
            pltpu.VMEM((width, width), BF16),
            pltpu.VMEM((2, batch, 16, channels), F32),
            pltpu.VMEM((2, 2, batch, 16, channels), BF16),
            pltpu.VMEM((2, 2, batch, 16, channels), BF16),
            pltpu.VMEM((2, 2, 16, channels), F32),
            pltpu.VMEM((2, 2, 16, channels), BF16),
            pltpu.VMEM((2, 2, 16, channels), BF16),
            pltpu.VMEM((2, 3, 2, batch * 16, channels), F32),
            dma((2,)),
            dma,
            dma,
            dma((2,)),
            dma((2,)),
            dma((2,)),
            dma((2, 2)),
            dma((2,)),
            dma((2,)),
            dma,
            dma,
            dma((2, rows + 1)),
        ],
        compiler_params=pltpu.CompilerParams(
            collective_id=0, has_side_effects=True, vmem_limit_bytes=40 * 1024 * 1024
        ),
    )(*(pltpu.with_memory_space_constraint(x, pltpu.HBM) for x in arguments))
    return jnp.swapaxes(flat, 2, 3)


def solution(mesh):
    return jax.shard_map(
        functools.partial(shards, mesh.shape["rows"]),
        mesh=mesh,
        in_specs=(P(None, "rows", "cols", None), P(None, "rows", "cols", None), P(), P()),
        out_specs=P(None, "rows", "cols", None),
        check_vma=False,
    )
```

```python
import functools
import math

import jax
import jax.numpy as jnp
from jax import lax
from jax.experimental import pallas as pl
from jax.experimental.pallas import tpu as pltpu
from jax.sharding import PartitionSpec as P

DISP = 256
LEVELS = 4
MESH = pl.DeviceIdType.MESH
F32 = jnp.float32
BF16 = jnp.bfloat16

DIRECT = 2
LAG = 3
EARLY = (3, 4, 5, 7, 8, 9, 11)
PAIRED = 9


def kernel(
    rows_total,
    left_hbm,
    right_hbm,
    weight_hbm,
    bias_hbm,
    result,
    buf,
    weight,
    bias,
    taps,
    enc,
    got,
    pool,
    flip,
    edge32,
    edge,
    halo,
    corner32,
    corner,
    halo_corner,
    extra,
    load_sem,
    weight_sem,
    bias_sem,
    row_send,
    row_recv,
    col_send,
    col_recv,
    corner_send,
    corner_recv,
    own_send,
    relay_send,
    got_recv,
):
    r = lax.axis_index("rows")
    c = lax.axis_index("cols")
    last = rows_total - 1
    batch, height, width, channels = left_hbm.shape
    images = (right_hbm, left_hbm)
    rows = batch * height
    inner = (height - 2) // 2
    chunks = rows // 2

    def place(j):
        is_inner = j < batch * inner
        b = jnp.where(is_inner, j // inner, j - batch * inner)
        first = jnp.where(is_inner, 1 + 2 * (j % inner), 0)
        second = jnp.where(is_inner, 2 + 2 * (j % inner), height - 1)
        return b, first, second

    def is_direct(k):
        return jnp.logical_and(k >= DIRECT, k < 2 * DIRECT)

    def round_about(u):
        return jnp.where(u < DIRECT, u, u + DIRECT)

    def place_row(k):
        b, first, second = place(k // 2)
        return b, jnp.where(k % 2 == 0, first, second)

    def load(image):
        return pltpu.make_async_copy(
            images[image], buf.at[image, :, pl.ds(1, height)], load_sem.at[image]
        )

    weight_copy = pltpu.make_async_copy(weight_hbm, weight, weight_sem)
    bias_copy = pltpu.make_async_copy(bias_hbm, bias, bias_sem)

    sends_col = (c < 3, c > 0)
    gets_col = (c > 0, c < 3)
    sends_row = (r < last, r > 0)
    gets_row = (r > 0, r < last)
    col_to = ((c + 1) % 4, (c + 3) % 4)
    row_to = (r + 1, r - 1)

    barrier = pltpu.get_barrier_semaphore()

    def greet(row, col):
        pl.semaphore_signal(
            barrier, inc=1, device_id={"rows": row, "cols": col}, device_id_type=MESH
        )

    for side in range(2):
        greet(r, col_to[side])
    for end in range(2):
        pl.when(sends_row[end])(functools.partial(greet, row_to[end], c))

    load(0).start()
    weight_copy.start()
    bias_copy.start()
    load(1).start()

    d = lax.broadcasted_iota(jnp.int32, (DISP - (DISP >> 3), 2 * DISP), 1) % DISP
    lane = lax.broadcasted_iota(jnp.int32, (DISP - (DISP >> 3), 2 * DISP), 0)
    table = jnp.zeros(d.shape, F32)
    start = 0
    for level in range(1, LEVELS):
        size = DISP >> level
        inside = jnp.logical_and(lane >= start, lane < start + size)
        hit = jnp.logical_and(inside, (d >> level) == lane - start)
        table = jnp.where(hit, 1.0 / (1 << level), table)
        start += size
    pool[...] = table.astype(BF16)
    i0 = lax.broadcasted_iota(jnp.int32, (width, width), 0)
    i1 = lax.broadcasted_iota(jnp.int32, (width, width), 1)
    flip[...] = jnp.where(i0 + i1 == width - 1, 1.0, 0.0).astype(BF16)

    @pl.when(r == 0)
    def _():
        buf[:, :, 0] = jnp.zeros((2, batch, width, channels), BF16)
        halo_corner[0] = jnp.zeros((2, 16, channels), BF16)

    @pl.when(r == last)
    def _():
        buf[:, :, height + 1] = jnp.zeros((2, batch, width, channels), BF16)
        halo_corner[1] = jnp.zeros((2, 16, channels), BF16)

    @pl.when(c == 0)
    def _():
        halo[0] = jnp.zeros(halo.shape[1:], BF16)

    @pl.when(c == 3)
    def _():
        halo[1] = jnp.zeros(halo.shape[1:], BF16)

    def take_column(image, b, row, side):
        if side == 0:
            return buf[image, b, row, width - 16 : width, :].astype(F32)[15:16]
        return buf[image, b, row, 0:16, :].astype(F32)[0:1]

    def extract(image):
        load(image).wait()
        for side in range(2):
            for b in range(batch):
                for h in range(height):
                    edge32[side, b, h + 1 : h + 2, :] = take_column(image, b, h + 1, side)
            edge[side, image] = edge32[side].astype(BF16)

    def column_copy(side, image):
        return pltpu.make_async_remote_copy(
            src_ref=edge.at[side, image],
            dst_ref=halo.at[side, image],
            send_sem=col_send.at[side],
            recv_sem=col_recv.at[side, image],
            device_id={"rows": r, "cols": col_to[side]},
            device_id_type=MESH,
        )

    def row_copy(side, image, b):
        source, target, to = (height - 1, 0, r + 1) if side == 0 else (0, height + 1, r - 1)
        return pltpu.make_async_remote_copy(
            src_ref=images[image].at[b, source],
            dst_ref=buf.at[image, b, target],
            send_sem=row_send.at[side],
            recv_sem=row_recv.at[side],
            device_id={"rows": to, "cols": c},
            device_id_type=MESH,
        )

    def row_copies(side):
        rows_sent = got.at[0, pl.ds(0, 2 * batch)]
        return pltpu.make_async_remote_copy(
            src_ref=rows_sent,
            dst_ref=rows_sent,
            send_sem=row_send.at[side],
            recv_sem=row_recv.at[side],
            device_id={"rows": row_to[side], "cols": c},
            device_id_type=MESH,
        )

    def column_copies(side):
        return pltpu.make_async_remote_copy(
            src_ref=edge.at[side],
            dst_ref=halo.at[side],
            send_sem=col_send.at[side],
            recv_sem=col_recv.at[side, 0],
            device_id={"rows": r, "cols": col_to[side]},
            device_id_type=MESH,
        )

    def corner_copy(end):
        return pltpu.make_async_remote_copy(
            src_ref=corner.at[end],
            dst_ref=halo_corner.at[end],
            send_sem=corner_send.at[end],
            recv_sem=corner_recv.at[end],
            device_id={"rows": row_to[end], "cols": c},
            device_id_type=MESH,
        )

    def each_col(conditions, action):
        for side in range(2):
            @pl.when(conditions[side])
            def _(side=side):
                action(side)

    def each_row(conditions, action):
        for side in range(2):
            @pl.when(conditions[side])
            def _(side=side):
                for image in range(2):
                    for b in range(batch):
                        action(side, image, b)

    extract(0)
    above = (r > 0).astype(jnp.int32) + (r < last).astype(jnp.int32)
    pl.semaphore_wait(barrier, 2 + above)
    each_col(sends_col, lambda side: column_copy(side, 0).start())
    each_row(sends_row, lambda side, image, b: row_copy(side, image, b).start())
    extract(1)
    each_col(sends_col, lambda side: column_copy(side, 1).start())
    def product(image, j, slot):
        b, first, second = place(j)
        parts = [
            jnp.concatenate([buf[image, b, first + tap], buf[image, b, second + tap]], axis=0)
            for tap in range(3)
        ]
        window = jnp.concatenate(parts, axis=1)
        for tap in range(3):
            matrix = weight[:, tap].reshape(3 * channels, channels)
            taps[slot, tap] = jnp.dot(window, matrix, preferred_element_type=F32)

    def from_halo(image):
        for side in range(2):
            vectors = halo[side, image].reshape(batch * 16, channels)
            for tap in range(3):
                extra[side, tap, image] = jnp.dot(
                    vectors, weight[tap, 2 * side], preferred_element_type=F32
                )

    def corners_out():
        each_col(gets_col, lambda side: column_copy(side, 1).wait_recv())
        for end in range(2):
            row = 1 if end else height
            for side in range(2):
                for image in range(2):
                    for b in range(batch):
                        at = image * batch + b
                        vector = halo[side, image, b].astype(F32)[row : row + 1]
                        corner32[end, side, at : at + 1, :] = vector
                corner[end, side] = corner32[end, side].astype(BF16)
        each_col(sends_row, lambda end: corner_copy(end).start())

    def corners_add(image):
        for side in range(2):
            for end in range(2):
                values = jnp.dot(
                    halo_corner[end, side], weight[2 * end, 2 * side], preferred_element_type=F32
                )
                for b in range(batch):
                    at = image * batch + b
                    to = b * 16 + end * (height + 1)
                    extra[side, 2 * end, image, to : to + 1, :] = values[at : at + 1]

    def corners_in():
        each_col(gets_row, lambda side: row_copies(side).wait_recv())
        each_col(gets_row, lambda end: corner_copy(end).wait_recv())
        corners_add(0)

    column = lax.broadcasted_iota(jnp.int32, (width, channels), 0)

    def encoded(image, b, h, slot, half):
        span = pl.ds(half * width, width)
        sides = [
            sum(extra[side, tap, image, pl.ds(b * 16 + h + tap, 1), :] for tap in range(3))
            for side in range(2)
        ]
        before = pltpu.roll(taps[slot, 0, span, :], 1, 0)
        after = pltpu.roll(taps[slot, 2, span, :], width - 1, 0)
        total = jnp.where(column == 0, sides[0], before) + taps[slot, 1, span, :]
        total = total + jnp.where(column == width - 1, sides[1], after) + bias[...]
        return (buf[image, b, h + 1].astype(F32) + jnp.maximum(total, 0.0)).astype(BF16)

    def piece(ref, which, f, part):
        if part is None:
            return ref.at[which, f]
        return ref.at[which, rows - 1, pl.ds(part * (width // 2), width // 2)]

    def landed(which, f, part):
        return got_recv.at[which, f if part is None else rows - 1 + part]

    def own_copy(k, f, part=None):
        to = jnp.where(c == 0, 1, jnp.where(c == 1, jnp.where(is_direct(k), 2, 0), 3))
        return pltpu.make_async_remote_copy(
            src_ref=piece(enc, 0, f, part),
            dst_ref=piece(got, 0, f, part),
            send_sem=own_send,
            recv_sem=landed(0, f, part),
            device_id={"rows": r, "cols": to},
            device_id_type=MESH,
        )

    def relay_copy(f, part=None):
        source = jnp.where(c == 3, 1, 0)
        target = jnp.where(c == 3, 0, 1)
        to = jnp.where(c == 0, 3, jnp.where(c == 2, 3, 2))
        return pltpu.make_async_remote_copy(
            src_ref=piece(got, source, f, part),
            dst_ref=piece(got, target, f, part),
            send_sem=relay_send,
            recv_sem=landed(target, f, part),
            device_id={"rows": r, "cols": to},
            device_id_type=MESH,
        )

    def arrival(which, f, part=None):
        return pltpu.make_async_remote_copy(
            src_ref=piece(got, which, f, part),
            dst_ref=piece(got, which, f, part),
            send_sem=relay_send,
            recv_sem=landed(which, f, part),
            device_id={"rows": r, "cols": (c + 1) % 4},
            device_id_type=MESH,
        )

    def in_pieces(condition, k, f, action):
        @pl.when(jnp.logical_and(condition, k < rows - 1))
        def _():
            action(f, None)

        @pl.when(jnp.logical_and(condition, k == rows - 1))
        def _():
            for part in range(2):
                action(f, part)

    def relays(k):
        direct = is_direct(k)
        return jnp.logical_or(
            c == 1,
            jnp.logical_or(
                jnp.logical_and(c == 2, direct),
                jnp.logical_and(jnp.logical_or(c == 0, c == 3), jnp.logical_not(direct)),
            ),
        )

    def tick(t):
        k = jnp.where(c == 0, round_about(t), jnp.where(c == 3, round_about(t - LAG), t))
        known = jnp.clip(k, 0, rows - 1)
        b, h = place_row(known)
        f = b * height + h

        def action(f, part):
            arrival(jnp.where(c == 3, 1, 0), f, part).wait_recv()
            relay_copy(f, part).start()

        in_pieces(jnp.logical_and(k == known, relays(known)), known, f, action)

    def correlate(steps):
        todo = []
        for step in steps:
            late = jnp.where(step < rows - DIRECT, round_about(step), step - (rows - 2 * DIRECT))
            k = jnp.where(c == 2, step, late)
            b, h = place_row(k)
            f = b * height + h
            direct = is_direct(k)

            near = jnp.logical_or(c == 3, jnp.logical_and(c == 2, jnp.logical_not(direct)))
            in_pieces(near, k, f, lambda f, part: arrival(0, f, part).wait_recv())
            distant = jnp.logical_or(c == 2, jnp.logical_and(c == 3, direct))
            in_pieces(distant, k, f, lambda f, part: arrival(1, f, part).wait_recv())
            todo.append((b, h, f))
        lower = i1 <= i0
        for b, h, f in todo:
            query = enc[1, f]
            blocks = []
            for distance, keys in enumerate((enc[0, f], got[0, f], got[1, f])):
                scores = lax.dot_general(
                    query, keys, (((1,), (1,)), ((), ())), preferred_element_type=F32
                )
                if distance:
                    scores = jnp.where(c >= distance, scores, 0.0)
                blocks.append(pltpu.roll(scores, 1, 1, stride=1, stride_axis=0))
            volume = jnp.concatenate(
                [
                    jnp.where(lower, blocks[0], blocks[1]).T,
                    jnp.where(lower, blocks[1], blocks[2]).T,
                ],
                axis=0,
            ) * (1.0 / math.sqrt(channels))
            high = volume.astype(BF16)
            low = (volume - high.astype(F32)).astype(BF16)
            result[b, h, 0:DISP, :] = volume
            result[b, h, DISP:, :] = jnp.dot(
                pool[...], jnp.concatenate([high, low], axis=0), preferred_element_type=F32
            )

    weight_copy.wait()
    bias_copy.wait()
    product(0, 0, 0)
    each_col(gets_col, lambda side: column_copy(side, 0).wait_recv())
    from_halo(0)

    def finish_right(j):
        slot = j % 2
        b, first, second = place(j)
        pair = [encoded(0, b, h, slot, half) for half, h in enumerate((first, second))]
        turned = jnp.dot(flip[...], jnp.concatenate(pair, axis=1), preferred_element_type=F32).astype(BF16)
        for half, h in enumerate((first, second)):
            enc[0, b * height + h] = turned[:, half * channels : (half + 1) * channels]

        for half, h in enumerate((first, second)):
            k = 2 * j + half
            in_pieces(c < 3, k, b * height + h, lambda f, part, k=k: own_copy(k, f, part).start())

    def right_chunk(j, _):
        @pl.when(j == 2)
        def _():
            corners_out()

        @pl.when(j == 9)
        def _():
            corners_in()

        following = j + 1
        product(following // chunks, following % chunks, 1 - j % 2)
        finish_right(j)
        for t, at in enumerate(EARLY):
            pl.when(j == at)(functools.partial(tick, t))
        return 0

    finish_right(0)
    product(0, 1, 1)
    lax.fori_loop(1, chunks, right_chunk, 0)
    from_halo(1)
    corners_add(1)

    early = len(EARLY) + chunks // 2

    def left_chunk(j, _):
        slot = (chunks + j) % 2
        product(1, jnp.minimum(j + 1, chunks - 1), 1 - slot)
        b, first, second = place(j)
        for half, h in enumerate((first, second)):
            enc[1, b * height + h] = encoded(1, b, h, slot, half)

        @pl.when(j % 2 == 0)
        def _():
            tick(len(EARLY) + j // 2)

        return 0

    lax.fori_loop(0, chunks, left_chunk, 0)

    def paired(s, _):
        tick(early + s)
        correlate((2 * s, 2 * s + 1))
        return 0

    def single(step, _):
        tick(early - PAIRED + step)
        correlate((step,))
        return 0

    lax.fori_loop(0, PAIRED, paired, 0)
    lax.fori_loop(2 * PAIRED, rows, single, 0)

    each_col(sends_col, lambda side: column_copies(side).wait_send())
    each_col(sends_row, lambda side: row_copies(side).wait_send())
    each_col(sends_row, lambda end: corner_copy(end).wait_send())

    def drain(sem, count):
        rows_sent = got.at[0, pl.ds(0, count)]
        pltpu.make_async_remote_copy(
            src_ref=rows_sent,
            dst_ref=rows_sent,
            send_sem=sem,
            recv_sem=got_recv.at[0, 0],
            device_id={"rows": r, "cols": (c + 1) % 4},
            device_id_type=MESH,
        ).wait_send()

    pl.when(c < 3)(lambda: drain(own_send, rows))
    pl.when(c == 1)(lambda: drain(relay_send, rows))
    pl.when(c == 2)(lambda: drain(relay_send, DIRECT))
    pl.when(jnp.logical_or(c == 0, c == 3))(lambda: drain(relay_send, rows - DIRECT))


def shards(rows_total, left_features, right_features, conv_weight, conv_bias):
    batch, height, width, channels = left_features.shape
    rows = batch * height
    lanes = sum(DISP >> level for level in range(LEVELS))
    far = pl.BlockSpec(memory_space=pltpu.HBM)
    near = pl.BlockSpec(memory_space=pltpu.VMEM)
    dma = pltpu.SemaphoreType.DMA
    arguments = (left_features, right_features, conv_weight, conv_bias.reshape(1, channels))
    flat = pl.pallas_call(
        functools.partial(kernel, rows_total),
        out_shape=pltpu.VMEM((batch, height, lanes, width), F32),
        in_specs=[far] * 4,
        out_specs=near,
        scratch_shapes=[
            pltpu.VMEM((2, batch, height + 2, width, channels), BF16),
            pltpu.VMEM((3, 3, channels, channels), BF16),
            pltpu.VMEM((1, channels), F32),
            pltpu.VMEM((2, 3, 2 * width, channels), F32),
            pltpu.VMEM((2, rows, width, channels), BF16),
            pltpu.VMEM((2, rows, width, channels), BF16),
            pltpu.VMEM((lanes - DISP, 2 * DISP), BF16),
            pltpu.VMEM((width, width), BF16),
            pltpu.VMEM((2, batch, 16, channels), F32),
            pltpu.VMEM((2, 2, batch, 16, channels), BF16),
            pltpu.VMEM((2, 2, batch, 16, channels), BF16),
            pltpu.VMEM((2, 2, 16, channels), F32),
            pltpu.VMEM((2, 2, 16, channels), BF16),
            pltpu.VMEM((2, 2, 16, channels), BF16),
            pltpu.VMEM((2, 3, 2, batch * 16, channels), F32),
            dma((2,)),
            dma,
            dma,
            dma((2,)),
            dma((2,)),
            dma((2,)),
            dma((2, 2)),
            dma((2,)),
            dma((2,)),
            dma,
            dma,
            dma((2, rows + 1)),
        ],
        compiler_params=pltpu.CompilerParams(
            collective_id=0, has_side_effects=True, vmem_limit_bytes=40 * 1024 * 1024
        ),
    )(*(pltpu.with_memory_space_constraint(x, pltpu.HBM) for x in arguments))
    return jnp.swapaxes(flat, 2, 3)


def solution(mesh):
    return jax.shard_map(
        functools.partial(shards, mesh.shape["rows"]),
        mesh=mesh,
        in_specs=(P(None, "rows", "cols", None), P(None, "rows", "cols", None), P(), P()),
        out_specs=P(None, "rows", "cols", None),
        check_vma=False,
    )
```
